32 devices in a mesh: dp: 1 (over z), tp: 4 (over y), sq: 8 (over x, core).
Axes of the slice: x: 4, y: 4, z: 1, core: 2. Of those that a mesh axis runs over, the one named last changes fastest.
The devices are a block of a 4x4x8 slice.
Arguments:
- hidden: bfloat16 [256, 2048], P('dp')
- cache_lens: int32 [256], P('dp')
- k_cache: bfloat16 [256, 2048, 128], P('dp', 'sq')
- v_cache: bfloat16 [256, 2048, 128], P('dp', 'sq')
- ln_gain: float32 [2048], replicated
- ln_bias: float32 [2048], replicated
- w_query: bfloat16 [2048, 2048], P(None, 'tp')
- b_query: float32 [2048], P('tp')
- w_kv: bfloat16 [2048, 256], replicated
- b_kv: float32 [256], replicated
- w_out: bfloat16 [2048, 2048], P('tp')
- b_out: float32 [2048], replicated
Outputs:
- output 1: bfloat16 [256, 2048], P('dp')
- output 2: bfloat16 [256, 2048, 128], P('dp', 'sq')
- output 3: bfloat16 [256, 2048, 128], P('dp', 'sq')
All inputs are finite; a program needn't handle non-finite values.
Results may differ from the reference program's by a relative error of at most 0.0034095.
Values sent between devices are 32-bit elements.
A program may use at most 768 MiB of HBM per device.

```python
import math
import jax
import jax.numpy as jnp
from jax import lax

BATCH = 256
CACHE_LEN = 2048
D_MODEL = 2048
HEADS = 16
HEAD_DIM = 128


def layer_norm(x_rows, ln_gain, ln_bias):
    x_wide = x_rows.astype(jnp.float32)
    mean_val = jnp.mean(x_wide, axis=-1, keepdims=True)
    centered = x_wide - mean_val
    variance = jnp.mean(centered * centered, axis=-1, keepdims=True)
    normed = centered * lax.rsqrt(variance + 1e-5)
    return (normed * ln_gain + ln_bias).astype(jnp.bfloat16)


def setup_inputs(seed: int = 0, part: int = 0) -> dict:
    own_keys = jax.random.split(jax.random.fold_in(jax.random.key(seed), part), 5)
    shared_keys = jax.random.split(jax.random.key(seed + 1), 10)
    q_width = HEADS * HEAD_DIM
    score_var = max(1.0, math.log(CACHE_LEN / 32.0))
    key_scale = math.sqrt(score_var / 2.0)
    self_bias = (math.log(0.6 * CACHE_LEN) + 0.5 * score_var) / math.sqrt(HEAD_DIM)
    hidden = jax.random.normal(own_keys[0], (BATCH, D_MODEL), jnp.float32).astype(jnp.bfloat16)
    drawn = CACHE_LEN - 1 - jax.random.randint(own_keys[1], (BATCH,), 0, CACHE_LEN // 2)
    order = jax.random.permutation(own_keys[2], BATCH)
    seq_ids = jnp.arange(BATCH)
    cache_lens = jnp.where(seq_ids == order[0], CACHE_LEN - 1, jnp.where(seq_ids == order[1], 1, drawn)).astype(jnp.int32)
    k_cache = (key_scale * jax.random.normal(own_keys[3], (BATCH, CACHE_LEN, HEAD_DIM), jnp.float32)).astype(jnp.bfloat16)
    v_cache = jax.random.normal(own_keys[4], (BATCH, CACHE_LEN, HEAD_DIM), jnp.float32).astype(jnp.bfloat16)
    ln_gain = 1.0 + 0.3 * jax.random.normal(shared_keys[0], (D_MODEL,), jnp.float32)
    ln_bias = 0.3 * jax.random.normal(shared_keys[1], (D_MODEL,), jnp.float32)
    w_query = (jax.random.normal(shared_keys[2], (D_MODEL, q_width), jnp.float32) * D_MODEL ** -0.5).astype(jnp.bfloat16)
    shared_dir = jax.random.normal(shared_keys[3], (HEAD_DIM,), jnp.float32)
    b_query = jnp.tile(shared_dir, HEADS) + 0.2 * jax.random.normal(shared_keys[4], (q_width,), jnp.float32)
    w_kv = (jax.random.normal(shared_keys[5], (D_MODEL, 2 * HEAD_DIM), jnp.float32) * D_MODEL ** -0.5).astype(jnp.bfloat16)
    key_bias = self_bias * shared_dir + 0.2 * jax.random.normal(shared_keys[6], (HEAD_DIM,), jnp.float32)
    val_bias = 0.5 * jax.random.normal(shared_keys[7], (HEAD_DIM,), jnp.float32)
    b_kv = jnp.concatenate([key_bias, val_bias])
    w_out = (jax.random.normal(shared_keys[8], (q_width, D_MODEL), jnp.float32) * q_width ** -0.5).astype(jnp.bfloat16)
    b_out = 0.3 * jax.random.normal(shared_keys[9], (D_MODEL,), jnp.float32)
    return {"hidden": hidden, "cache_lens": cache_lens, "k_cache": k_cache, "v_cache": v_cache, "ln_gain": ln_gain, "ln_bias": ln_bias, "w_query": w_query, "b_query": b_query, "w_kv": w_kv, "b_kv": b_kv, "w_out": w_out, "b_out": b_out}


def reference(hidden, cache_lens, k_cache, v_cache, ln_gain, ln_bias, w_query, b_query, w_kv, b_kv, w_out, b_out):
    normed = layer_norm(hidden, ln_gain, ln_bias)
    query = (jnp.dot(normed, w_query, preferred_element_type=jnp.float32) + b_query).astype(jnp.bfloat16)
    query = query.reshape(BATCH, HEADS, HEAD_DIM)
    key_val = (jnp.dot(normed, w_kv, preferred_element_type=jnp.float32) + b_kv).astype(jnp.bfloat16)
    positions = jnp.arange(CACHE_LEN, dtype=jnp.int32)
    at_slot = (positions[None, :] == cache_lens[:, None])[:, :, None]
    key_new = jnp.where(at_slot, key_val[:, None, :HEAD_DIM], k_cache)
    val_new = jnp.where(at_slot, key_val[:, None, HEAD_DIM:], v_cache)

    def one_sequence(packed):
        query_row, key_rows, val_rows, length = packed
        scores = jnp.einsum("nd,td->nt", query_row.astype(jnp.float32), key_rows.astype(jnp.float32)) * (HEAD_DIM ** -0.5)
        valid = positions <= length
        scores = jnp.where(valid[None, :], scores, -jnp.inf)
        weights = jax.nn.softmax(scores, axis=-1)
        return jnp.einsum("nt,td->nd", weights, val_rows.astype(jnp.float32)).astype(jnp.bfloat16)

    attended = lax.map(one_sequence, (query, key_new, val_new, cache_lens))
    projected = jnp.dot(attended.reshape(BATCH, HEADS * HEAD_DIM), w_out, preferred_element_type=jnp.float32)
    out_hidden = (hidden.astype(jnp.float32) + projected + b_out).astype(jnp.bfloat16)
    return (out_hidden, key_new, val_new)
```

```python
import functools
import jax
import jax.numpy as jnp
from jax import lax
from jax.sharding import PartitionSpec as P
from jax.experimental import pallas as pl
from jax.experimental.pallas import tpu as pltpu

F32 = jnp.float32
BF16 = jnp.bfloat16
MESH = pl.DeviceIdType.MESH
CHUNK = 16
LOW = -1e30


def attend_kernel(lens, hid_h, gain, bias, wq_h, bq, wkv_h, bkv, k_in, v_in,
                  k_out, v_out, num, stat,
                  hid, wq, wkv, h_scr, kv_scr, qd, kbuf, vbuf, wsem, ksem, vsem, kosem, vosem):
    batch, pos, dim = k_in.shape
    heads = wq.shape[1] // dim
    chunks = batch // CHUNK
    first = lax.axis_index("sq") * pos

    wcopies = [pltpu.make_async_copy(src, dst, wsem.at[i])
               for i, (src, dst) in enumerate(((hid_h, hid), (wkv_h, wkv), (wq_h, wq)))]

    def rd(c, src, buf, sem):
        part = pl.ds(c * CHUNK, CHUNK)
        return pltpu.make_async_copy(src.at[part], buf.at[part], sem.at[c])

    def wr(c, buf, dst, sem):
        part = pl.ds(c * CHUNK, CHUNK)
        return pltpu.make_async_copy(buf.at[part], dst.at[part], sem.at[c])

    for copy in wcopies:
        copy.start()
    for c in range(chunks):
        rd(c, k_in, kbuf, ksem).start()
        rd(c, v_in, vbuf, vsem).start()

    wcopies[0].wait()
    rows = 32

    def norm_rows(i, _):
        part = pl.ds(pl.multiple_of(i * rows, rows), rows)
        wide = hid[part, :].astype(F32)
        mean = jnp.mean(wide, axis=-1, keepdims=True)
        cent = wide - mean
        var = jnp.mean(cent * cent, axis=-1, keepdims=True)
        normed = cent * lax.rsqrt(var + 1e-5)
        h_scr[part, :] = (normed * gain[...] + bias[...]).astype(BF16)
        return 0

    lax.fori_loop(0, batch // rows, norm_rows, 0)
    wcopies[1].wait()
    kv = jnp.dot(h_scr[...], wkv[...], preferred_element_type=F32) + bkv[...]
    kv_scr[...] = kv.astype(BF16).astype(F32)
    wcopies[2].wait()
    qd[...] = jnp.zeros_like(qd)
    for h in range(heads):
        cols = slice(h * dim, (h + 1) * dim)
        q = jnp.dot(h_scr[...], wq[:, cols], preferred_element_type=F32) + bq[:, cols]
        q = q.astype(BF16).astype(F32).reshape(batch // 2, 2, dim)
        qd[:, h, 0:dim] = q[:, 0, :]
        qd[:, heads + h, dim:2 * dim] = q[:, 1, :]

    pair_rows = 2 * heads
    row = lax.broadcasted_iota(jnp.int32, (pair_rows, pos), 0)
    at = first + lax.broadcasted_iota(jnp.int32, (pair_rows, pos), 1)
    tile_row = lax.broadcasted_iota(jnp.int32, (16, dim), 0)
    lane = lax.broadcasted_iota(jnp.int32, (pair_rows, dim), 1)
    low_half = lax.broadcasted_iota(jnp.int32, (pair_rows, dim), 0) < heads

    def step(c, _):
        rd(c, k_in, kbuf, ksem).wait()
        rd(c, v_in, vbuf, vsem).wait()
        base = c * CHUNK
        patched = []
        for i in range(CHUNK):
            slot = lens[base + i] - first
            start = pl.multiple_of((jnp.clip(slot, 0, pos - 1) // 16) * 16, 16)
            hit = tile_row + start == slot
            new = kv_scr[pl.ds(base + i, 1), :]
            kt = kbuf[base + i, pl.ds(start, 16), :].astype(F32)
            vt = vbuf[base + i, pl.ds(start, 16), :].astype(F32)
            patched.append((start, jnp.where(hit, new[:, :dim], kt).astype(BF16),
                            jnp.where(hit, new[:, dim:], vt).astype(BF16)))
        for i, (start, kt, vt) in enumerate(patched):
            kbuf[base + i, pl.ds(start, 16), :] = kt
            vbuf[base + i, pl.ds(start, 16), :] = vt
        wr(c, kbuf, k_out, kosem).start()
        wr(c, vbuf, v_out, vosem).start()
        scores = []
        for p in range(CHUNK // 2):
            b = base + 2 * p
            keys = jnp.concatenate([kbuf[b], kbuf[b + 1]], axis=1)
            lhs = qd[c * (CHUNK // 2) + p].astype(BF16)
            s = lax.dot_general(lhs, keys, (((1,), (1,)), ((), ())), preferred_element_type=F32)
            scores.append(s * (dim ** -0.5))
        parts = []
        for p in range(CHUNK // 2):
            b = base + 2 * p
            valid = at <= jnp.where(row < heads, lens[b], lens[b + 1])
            s = jnp.where(valid, scores[p], LOW)
            m = jnp.max(s, axis=-1, keepdims=True)
            w = jnp.where(valid, jnp.exp(s - m), 0.0)
            total = jnp.sum(w, axis=-1, keepdims=True)
            parts.append((m, total, w.astype(BF16)))
        for p in range(CHUNK // 2):
            b = base + 2 * p
            m, total, w = parts[p]
            vals = jnp.concatenate([vbuf[b], vbuf[b + 1]], axis=1)
            o = jnp.dot(w, vals, preferred_element_type=F32)
            out = pl.ds(pl.multiple_of(b * heads, pair_rows), pair_rows)
            num[out, :] = jnp.where(low_half, o[:, :dim], o[:, dim:])
            stat[out, :] = jnp.where(lane == 0, m, total)
        return 0

    lax.fori_loop(0, chunks, step, 0)
    for c in range(chunks):
        wr(c, kbuf, k_out, kosem).wait()
        wr(c, vbuf, v_out, vosem).wait()


def attend(cache_lens, hidden, ln_gain, ln_bias, w_query, b_query, w_kv, b_kv, k_cache, v_cache):
    batch, pos, dim = k_cache.shape
    width = hidden.shape[1]
    heads = w_query.shape[1] // dim
    chunks = batch // CHUNK
    vm = pl.BlockSpec(memory_space=pltpu.VMEM)
    anyw = pl.BlockSpec(memory_space=pl.ANY)
    dma = pltpu.SemaphoreType.DMA
    return pl.pallas_call(
        attend_kernel,
        in_specs=[pl.BlockSpec(memory_space=pltpu.SMEM), anyw, vm, vm, anyw, vm, anyw, vm, anyw, anyw],
        out_specs=[anyw, anyw, vm, vm],
        out_shape=[jax.ShapeDtypeStruct(k_cache.shape, k_cache.dtype),
                   jax.ShapeDtypeStruct(v_cache.shape, v_cache.dtype),
                   jax.ShapeDtypeStruct((batch * heads, dim), F32),
                   jax.ShapeDtypeStruct((batch * heads, dim), F32)],
        scratch_shapes=[
            pltpu.VMEM(hidden.shape, BF16), pltpu.VMEM(w_query.shape, BF16), pltpu.VMEM(w_kv.shape, BF16),
            pltpu.VMEM(hidden.shape, BF16), pltpu.VMEM((batch, 2 * dim), F32),
            pltpu.VMEM((batch // 2, 2 * heads, 2 * dim), F32),
            pltpu.VMEM(k_cache.shape, BF16), pltpu.VMEM(v_cache.shape, BF16),
            dma((3,)), dma((chunks,)), dma((chunks,)), dma((chunks,)), dma((chunks,)),
        ],
        compiler_params=pltpu.CompilerParams(vmem_limit_bytes=54 << 20),
        cost_estimate=pl.CostEstimate(flops=2 * batch * pos * dim * heads * 4, bytes_accessed=4 * k_cache.size * 2, transcendentals=0),
        name="attend",
    )(cache_lens, hidden, ln_gain.reshape(1, -1), ln_bias.reshape(1, -1), w_query, b_query.reshape(1, -1),
      w_kv, b_kv.reshape(1, -1), k_cache, v_cache)


def solution(mesh):
    def local_step(hidden, cache_lens, k_cache, v_cache, ln_gain, ln_bias, w_query, b_query, w_kv, b_kv, w_out, b_out):
        batch, pos, dim = k_cache.shape
        heads = w_query.shape[1] // dim
        key_new, val_new, num, stat = attend(cache_lens, hidden, ln_gain, ln_bias, w_query, b_query, w_kv, b_kv, k_cache, v_cache)
        m, total = stat[:, 0:1], stat[:, 1:2]
        top = lax.pmax(m, "sq")
        f = jnp.exp(m - top)
        den = lax.psum(total * f, "sq")
        numer = lax.psum(num * f, "sq")
        att = (numer / den).astype(BF16).reshape(batch, heads * dim)
        projected = lax.psum(jnp.dot(att, w_out, preferred_element_type=F32), "tp")
        out_hidden = (hidden.astype(F32) + projected + b_out).astype(BF16)
        return out_hidden, key_new, val_new

    cache_spec = P("dp", "sq", None)
    row_spec = P("dp", None)
    in_specs = (row_spec, P("dp"), cache_spec, cache_spec, P(None), P(None), P(None, "tp"), P("tp"), P(None, None), P(None), P("tp", None), P(None))
    return jax.shard_map(local_step, mesh=mesh, in_specs=in_specs, out_specs=(row_spec, cache_spec, cache_spec), check_vma=False)
```

```python
import functools
import jax
import jax.numpy as jnp
from jax import lax
from jax.sharding import PartitionSpec as P
from jax.experimental import pallas as pl
from jax.experimental.pallas import tpu as pltpu

F32 = jnp.float32
BF16 = jnp.bfloat16
MESH = pl.DeviceIdType.MESH
CHUNK = 16
GROUPS = 4
LOW = -1e30


def attend_kernel(n_sq, lens, hid_h, gain, bias, wq_h, bq, wkv_h, bkv, k_in, v_in,
                  k_out, v_out, msg,
                  hid, wq, wkv, h_scr, kv_scr, qd, stat, k_vm, v_vm, wsem, ksem, vsem, kosem, vosem):
    batch, pos, dim = k_in.shape
    heads = wq.shape[1] // dim
    chunks = batch // CHUNK
    per_group = batch // GROUPS
    own = per_group // n_sq
    rows = own * heads
    first = lax.axis_index("sq") * pos

    wcopies = [pltpu.make_async_copy(src, dst, wsem.at[i])
               for i, (src, dst) in enumerate(((hid_h, hid), (wkv_h, wkv), (wq_h, wq)))]

    def rd(i, src, buf, sem):
        span = pl.ds(i * CHUNK, CHUNK)
        return pltpu.make_async_copy(src.at[span], buf.at[span], sem.at[i])

    def wr(i, buf, dst, sem):
        span = pl.ds(i * CHUNK, CHUNK)
        return pltpu.make_async_copy(buf.at[span], dst.at[span], sem.at[i])

    for copy in wcopies:
        copy.start()
    for i in range(chunks):
        rd(i, k_in, k_vm, ksem).start()
        rd(i, v_in, v_vm, vsem).start()

    wcopies[0].wait()
    nrow = 32

    def norm_rows(i, _):
        span = pl.ds(pl.multiple_of(i * nrow, nrow), nrow)
        wide = hid[span, :].astype(F32)
        mean = jnp.mean(wide, axis=-1, keepdims=True)
        cent = wide - mean
        var = jnp.mean(cent * cent, axis=-1, keepdims=True)
        normed = cent * lax.rsqrt(var + 1e-5)
        h_scr[span, :] = (normed * gain[...] + bias[...]).astype(BF16)
        return 0

    lax.fori_loop(0, batch // nrow, norm_rows, 0)
    wcopies[1].wait()
    kv = jnp.dot(h_scr[...], wkv[...], preferred_element_type=F32) + bkv[...]
    kv_scr[...] = kv.astype(BF16).astype(F32)
    wcopies[2].wait()
    qd[...] = jnp.zeros_like(qd)
    for h in range(heads):
        span = slice(h * dim, (h + 1) * dim)
        q = jnp.dot(h_scr[...], wq[:, span], preferred_element_type=F32) + bq[:, span]
        q = q.astype(BF16).astype(F32).reshape(batch // 2, 2, dim)
        qd[:, h, 0:dim] = q[:, 0, :]
        qd[:, heads + h, dim:2 * dim] = q[:, 1, :]

    pair_rows = 2 * heads
    row = lax.broadcasted_iota(jnp.int32, (pair_rows, pos), 0)
    at = first + lax.broadcasted_iota(jnp.int32, (pair_rows, pos), 1)
    tile_row = lax.broadcasted_iota(jnp.int32, (16, dim), 0)
    lane = lax.broadcasted_iota(jnp.int32, (pair_rows, dim), 1)
    low_half = lax.broadcasted_iota(jnp.int32, (pair_rows, dim), 0) < heads
    pairs = CHUNK // 2
    scale = dim ** -0.5
    per = per_group // CHUNK
    block = dim // rows

    def attend(i, _):
        rd(i, k_in, k_vm, ksem).wait()
        rd(i, v_in, v_vm, vsem).wait()
        base = i * CHUNK
        grp = i // per
        tiles = []
        for j in range(CHUNK):
            slot = lens[base + j] - first
            start = pl.multiple_of((jnp.clip(slot, 0, pos - 1) // 16) * 16, 16)
            hit = tile_row + start == slot
            new = kv_scr[pl.ds(base + j, 1), :]
            kt = k_vm[base + j, pl.ds(start, 16), :].astype(F32)
            vt = v_vm[base + j, pl.ds(start, 16), :].astype(F32)
            tiles.append((start, jnp.where(hit, new[:, :dim], kt).astype(BF16),
                          jnp.where(hit, new[:, dim:], vt).astype(BF16)))
        for j, (start, kt, vt) in enumerate(tiles):
            k_vm[base + j, pl.ds(start, 16), :] = kt
            v_vm[base + j, pl.ds(start, 16), :] = vt
        wr(i, k_vm, k_out, kosem).start()
        wr(i, v_vm, v_out, vosem).start()
        scores = []
        for p in range(pairs):
            b = base + 2 * p
            keys = jnp.concatenate([k_vm[b], k_vm[b + 1]], axis=1)
            q = qd[i * pairs + p].astype(BF16)
            scores.append(lax.dot_general(q, keys, (((1,), (1,)), ((), ())), preferred_element_type=F32) * scale)
        weights = []
        for p in range(pairs):
            b = base + 2 * p
            valid = at <= jnp.where(row < heads, lens[b], lens[b + 1])
            sc = jnp.where(valid, scores[p], LOW)
            m = jnp.max(sc, axis=-1, keepdims=True)
            w = jnp.where(valid, jnp.exp(sc - m), 0.0)
            weights.append((m, jnp.sum(w, axis=-1, keepdims=True), w.astype(BF16)))
        for p in range(pairs):
            b = base + 2 * p
            m, total, w = weights[p]
            vals = jnp.concatenate([v_vm[b], v_vm[b + 1]], axis=1)
            o = jnp.dot(w, vals, preferred_element_type=F32)
            j = lax.rem(b, per_group)
            msg[grp, j // own, pl.ds(pl.multiple_of(lax.rem(j, own) * heads, pair_rows), pair_rows), :] = jnp.where(low_half, o[:, :dim], o[:, dim:])
            stat[pl.ds(pl.multiple_of(j * heads, pair_rows), pair_rows), :] = jnp.where(lane == 0, m, total)
        return 0

    for g in range(GROUPS):
        lax.fori_loop(g * per, (g + 1) * per, attend, 0)
        for a in range(n_sq // block):
            tile = stat[a * dim:(a + 1) * dim, :].T[0:8, :]
            for k in range(block):
                msg[g, a * block + k, rows:rows + 8, :] = tile
    for i in range(chunks):
        wr(i, k_vm, k_out, kosem).wait()
        wr(i, v_vm, v_out, vosem).wait()


def merge_kernel(n_tp, n_sq, heads, msg, wo, y_out, got, fac, att, part, got3,
                 s12, r12, s3, r3, s4a, r4a, s4b, r4b, s4c, r4c):
    dim = msg.shape[-1]
    own, width = part.shape[1:]
    rows = own * heads
    cols = width // n_tp
    n_x = n_sq // 2
    s = lax.axis_index("sq")
    t = lax.axis_index("tp")
    x, c = s // 2, lax.rem(s, 2)

    def sq_peer(i):
        return lax.rem(s + i, n_sq)

    def x_peer(i):
        return lax.rem(x + i, n_x) * 2 + c

    def y_peer(i):
        return lax.rem(t + i, n_tp)

    barrier = pltpu.get_barrier_semaphore()
    for i in range(1, n_sq):
        pl.semaphore_signal(barrier, inc=1, device_id={"sq": sq_peer(i)}, device_id_type=MESH)
    for i in range(1, n_tp):
        pl.semaphore_signal(barrier, inc=1, device_id={"tp": y_peer(i)}, device_id_type=MESH)
    pl.semaphore_wait(barrier, n_sq - 1 + n_tp - 1)

    block = dim // rows

    def copy12(g, i):
        return pltpu.make_async_remote_copy(msg.at[g, sq_peer(i)], got.at[g, i], s12.at[g, i], r12.at[g, i],
                                            device_id={"sq": sq_peer(i)}, device_id_type=MESH)

    def send12(g):
        for i in range(1, n_sq):
            copy12(g, i).start()

    def copy3(g, i):
        span = pl.ds(pl.multiple_of(y_peer(i) * cols, cols), cols)
        return pltpu.make_async_remote_copy(part.at[g, :, span], got3.at[g, i], s3.at[g, i], r3.at[g, i],
                                            device_id={"tp": y_peer(i)}, device_id_type=MESH)

    def proc12(g):
        for i in range(1, n_sq):
            copy12(g, i).wait_recv()
        tiles = [msg[g, s, rows:rows + 8, :]] + [got[g, i, rows:rows + 8, :] for i in range(1, n_sq)]
        m = jnp.concatenate([v[0:1] for v in tiles], axis=0)
        total = jnp.concatenate([v[1:2] for v in tiles], axis=0)
        f = jnp.exp(m - jnp.max(m, axis=0, keepdims=True))
        f = f / jnp.sum(f * total, axis=0, keepdims=True)
        fac[...] = jnp.concatenate([f, jnp.zeros((dim - n_sq, dim), F32)], axis=0).T
        fcol = fac[pl.ds(pl.multiple_of(lax.rem(s, block) * rows, rows), rows), :]
        a = msg[g, s, 0:rows, :] * fcol[:, 0:1]
        for i in range(1, n_sq):
            a = a + got[g, i, 0:rows, :] * fcol[:, i:i + 1]
        att[...] = a
        lhs = jnp.concatenate([att[pl.ds(h, own, stride=heads), :] for h in range(heads)], axis=1).astype(BF16)
        part[g] = jnp.dot(lhs, wo[...], preferred_element_type=F32)
        for i in range(1, n_tp):
            copy3(g, i).start()

    mine = pl.ds(pl.multiple_of(t * cols, cols), cols)

    def copy4a(g, i):
        if g % 2 == 0:
            to = {"sq": x_peer(i)}
        else:
            to = {"tp": y_peer(i)}
        ref = y_out.at[g, x, c, :, mine]
        return pltpu.make_async_remote_copy(ref, ref, s4a.at[g, i], r4a.at[g, i], device_id=to, device_id_type=MESH)

    def from4a(g, i):
        if g % 2 == 0:
            ref = y_out.at[g, lax.rem(x + n_x - i, n_x), c, :, mine]
            to = {"sq": x_peer(i)}
        else:
            src = lax.rem(t + n_tp - i, n_tp)
            ref = y_out.at[g, x, c, :, pl.ds(pl.multiple_of(src * cols, cols), cols)]
            to = {"tp": y_peer(i)}
        return pltpu.make_async_remote_copy(ref, ref, s4a.at[g, i], r4a.at[g, i], device_id=to, device_id_type=MESH)

    def strip(g, i):
        if g % 2 == 0:
            src = lax.rem(t + n_tp - i, n_tp)
            return y_out.at[g, :, c, :, pl.ds(pl.multiple_of(src * cols, cols), cols)]
        return y_out.at[g, lax.rem(x + n_x - i, n_x), c]

    def copy4b(g, i, ref):
        to = {"tp": y_peer(i)} if g % 2 == 0 else {"sq": x_peer(i)}
        return pltpu.make_async_remote_copy(ref, ref, s4b.at[g, i], r4b.at[g, i], device_id=to, device_id_type=MESH)

    def copy4c(g, i):
        ref = strip(g, i)
        return pltpu.make_async_remote_copy(ref, ref, s4c.at[g, i], r4c.at[g, i], device_id={"sq": s + 1 - 2 * c}, device_id_type=MESH)

    def from4c(g, i):
        if g % 2 == 0:
            src = lax.rem(t + n_tp - i, n_tp)
            ref = y_out.at[g, :, 1 - c, :, pl.ds(pl.multiple_of(src * cols, cols), cols)]
        else:
            ref = y_out.at[g, lax.rem(x + n_x - i, n_x), 1 - c]
        return pltpu.make_async_remote_copy(ref, ref, s4c.at[g, i], r4c.at[g, i], device_id={"sq": s + 1 - 2 * c}, device_id_type=MESH)

    def n_a(g):
        return n_x if g % 2 == 0 else n_tp

    def n_b(g):
        return n_tp if g % 2 == 0 else n_x

    def proc3(g):
        for i in range(1, n_tp):
            copy3(g, i).wait_recv()
        y = part[g, :, mine]
        for i in range(1, n_tp):
            y = y + got3[g, i]
        y_out[g, x, c, :, mine] = y
        for i in range(1, n_a(g)):
            copy4a(g, i).start()

    def fwd4(g):
        for i in range(1, n_a(g)):
            from4a(g, i).wait_recv()
        for i in range(1, n_b(g)):
            copy4b(g, i, strip(g, 0)).start()
        copy4c(g, 0).start()

    def end4(g):
        for i in range(1, n_b(g)):
            copy4b(g, i, strip(g, i)).wait_recv()
            copy4c(g, i).start()

    for g in range(GROUPS):
        send12(g)
    for g in range(GROUPS):
        proc12(g)
        if g >= 1:
            proc3(g - 1)
        if g >= 2:
            fwd4(g - 2)
        if g >= 3:
            end4(g - 3)
    proc3(GROUPS - 1)
    for g in range(GROUPS - 2, GROUPS):
        fwd4(g)
        end4(g - 1)
    end4(GROUPS - 1)
    for g in range(GROUPS):
        for i in range(n_b(g)):
            from4c(g, i).wait_recv()
    for g in range(GROUPS):
        for i in range(1, n_sq):
            copy12(g, i).wait_send()
        for i in range(1, n_tp):
            copy3(g, i).wait_send()
        for i in range(1, n_a(g)):
            copy4a(g, i).wait_send()
        for i in range(1, n_b(g)):
            copy4b(g, i, strip(g, 0)).wait_send()
        for i in range(n_b(g)):
            copy4c(g, i).wait_send()


VM = pl.BlockSpec(memory_space=pltpu.VMEM)
SM = pl.BlockSpec(memory_space=pltpu.SMEM)
ANYW = pl.BlockSpec(memory_space=pl.ANY)
DMA = pltpu.SemaphoreType.DMA


def attend(n_sq, cache_lens, hidden, ln_gain, ln_bias, w_query, b_query, w_kv, b_kv, k_cache, v_cache):
    batch, pos, dim = k_cache.shape
    heads = w_query.shape[1] // dim
    chunks = batch // CHUNK
    rows = batch // GROUPS // n_sq * heads
    return pl.pallas_call(
        functools.partial(attend_kernel, n_sq),
        in_specs=[SM, ANYW, VM, VM, ANYW, VM, ANYW, VM, ANYW, ANYW],
        out_specs=[ANYW, ANYW, VM],
        out_shape=[jax.ShapeDtypeStruct(k_cache.shape, BF16), jax.ShapeDtypeStruct(v_cache.shape, BF16),
                   pltpu.VMEM((GROUPS, n_sq, rows + 8, dim), F32)],
        scratch_shapes=[
            pltpu.VMEM(hidden.shape, BF16), pltpu.VMEM(w_query.shape, BF16), pltpu.VMEM(w_kv.shape, BF16),
            pltpu.VMEM(hidden.shape, BF16), pltpu.VMEM((batch, 2 * dim), F32),
            pltpu.VMEM((batch // 2, 2 * heads, 2 * dim), F32),
            pltpu.VMEM((batch // GROUPS * heads, dim), F32),
            pltpu.VMEM(k_cache.shape, BF16), pltpu.VMEM(v_cache.shape, BF16),
            DMA((3,)), *[DMA((chunks,)) for _ in range(4)],
        ],
        compiler_params=pltpu.CompilerParams(vmem_limit_bytes=54 << 20),
        cost_estimate=pl.CostEstimate(flops=4 * batch * pos * dim * heads * 2, bytes_accessed=4 * k_cache.size, transcendentals=0),
        name="attend",
    )(cache_lens, hidden, ln_gain.reshape(1, -1), ln_bias.reshape(1, -1), w_query, b_query.reshape(1, -1),
      w_kv, b_kv.reshape(1, -1), k_cache, v_cache)


def merge(n_tp, n_sq, batch, heads, msg, w_out):
    dim = msg.shape[-1]
    width = w_out.shape[1]
    own = batch // GROUPS // n_sq
    cols = width // n_tp
    sems = [DMA((GROUPS, n)) for n in (n_sq, n_sq, n_tp, n_tp) + (max(n_tp, n_sq // 2),) * 6]
    return pl.pallas_call(
        functools.partial(merge_kernel, n_tp, n_sq, heads),
        in_specs=[VM, VM],
        out_specs=VM,
        out_shape=pltpu.VMEM((GROUPS, n_sq // 2, 2, own, width), F32),
        scratch_shapes=[
            pltpu.VMEM(msg.shape, F32), pltpu.VMEM((dim, dim), F32), pltpu.VMEM((own * heads, dim), F32),
            pltpu.VMEM((GROUPS, own, width), F32), pltpu.VMEM((GROUPS, n_tp, own, cols), F32), *sems,
        ],
        compiler_params=pltpu.CompilerParams(collective_id=0, has_side_effects=True, vmem_limit_bytes=8 << 20),
        cost_estimate=pl.CostEstimate(flops=40 * batch * 256 * dim * heads, bytes_accessed=4 * batch * width, transcendentals=0),
        name="merge",
    )(msg, w_out)


def solution(mesh):
    n_tp, n_sq = mesh.shape["tp"], mesh.shape["sq"]

    def local_step(hidden, cache_lens, k_cache, v_cache, ln_gain, ln_bias, w_query, b_query, w_kv, b_kv, w_out, b_out):
        batch, pos, dim = k_cache.shape
        heads = w_query.shape[1] // dim
        key_new, val_new, msg = attend(n_sq, cache_lens, hidden, ln_gain, ln_bias, w_query, b_query, w_kv, b_kv, k_cache, v_cache)
        y = merge(n_tp, n_sq, batch, heads, msg, w_out)
        out_hidden = (hidden.astype(F32) + y.reshape(hidden.shape) + b_out).astype(BF16)
        return out_hidden, key_new, val_new

    cache_spec = P("dp", "sq", None)
    row_spec = P("dp", None)
    in_specs = (row_spec, P("dp"), cache_spec, cache_spec, P(None), P(None), P(None, "tp"), P("tp"), P(None, None), P(None), P("tp", None), P(None))
    return jax.shard_map(local_step, mesh=mesh, in_specs=in_specs, out_specs=(row_spec, cache_spec, cache_spec), check_vma=False)
```

```python
import functools
import jax
import jax.numpy as jnp
from jax import lax
from jax.sharding import PartitionSpec as P
from jax.experimental import pallas as pl
from jax.experimental.pallas import tpu as pltpu

F32 = jnp.float32
BF16 = jnp.bfloat16
MESH = pl.DeviceIdType.MESH
CHUNK = 16
DEPTH = 5
GROUPS = 2
LOW = -1e30


def attend_kernel(n_sq, lens, hid_h, gain, bias, wq_h, bq, wkv_h, bkv, k_in, v_in,
                  k_out, v_out, msg,
                  hid, wq, wkv, h_scr, kv_scr, qd, stat, k_vm, v_vm, wsem, ksem, vsem, kosem, vosem):
    batch, pos, dim = k_in.shape
    heads = wq.shape[1] // dim
    chunks = batch // CHUNK
    per_group = batch // GROUPS
    own = per_group // n_sq
    rows = own * heads
    first = lax.axis_index("sq") * pos

    wcopies = [pltpu.make_async_copy(src, dst, wsem.at[i])
               for i, (src, dst) in enumerate(((hid_h, hid), (wkv_h, wkv), (wq_h, wq)))]

    def rd(i, src, buf, sem):
        span = pl.ds(i * CHUNK, CHUNK)
        return pltpu.make_async_copy(src.at[span], buf.at[span], sem.at[i])

    def wr(i, buf, dst, sem):
        span = pl.ds(i * CHUNK, CHUNK)
        return pltpu.make_async_copy(buf.at[span], dst.at[span], sem.at[i])

    for copy in wcopies:
        copy.start()
    for i in range(DEPTH):
        rd(i, k_in, k_vm, ksem).start()
        rd(i, v_in, v_vm, vsem).start()

    wcopies[0].wait()
    nrow = 32

    def norm_rows(i, _):
        span = pl.ds(pl.multiple_of(i * nrow, nrow), nrow)
        wide = hid[span, :].astype(F32)
        mean = jnp.mean(wide, axis=-1, keepdims=True)
        cent = wide - mean
        var = jnp.mean(cent * cent, axis=-1, keepdims=True)
        normed = cent * lax.rsqrt(var + 1e-5)
        h_scr[span, :] = (normed * gain[...] + bias[...]).astype(BF16)
        return 0

    lax.fori_loop(0, batch // nrow, norm_rows, 0)
    wcopies[1].wait()
    kv = jnp.dot(h_scr[...], wkv[...], preferred_element_type=F32) + bkv[...]
    kv_scr[...] = kv.astype(BF16).astype(F32)
    wcopies[2].wait()
    qd[...] = jnp.zeros_like(qd)
    for h in range(heads):
        span = slice(h * dim, (h + 1) * dim)
        q = jnp.dot(h_scr[...], wq[:, span], preferred_element_type=F32) + bq[:, span]
        q = q.astype(BF16).astype(F32).reshape(batch // 2, 2, dim)
        qd[:, h, 0:dim] = q[:, 0, :]
        qd[:, heads + h, dim:2 * dim] = q[:, 1, :]

    pair_rows = 2 * heads
    row = lax.broadcasted_iota(jnp.int32, (pair_rows, pos), 0)
    at = first + lax.broadcasted_iota(jnp.int32, (pair_rows, pos), 1)
    tile_row = lax.broadcasted_iota(jnp.int32, (16, dim), 0)
    lane = lax.broadcasted_iota(jnp.int32, (pair_rows, dim), 1)
    low_half = lax.broadcasted_iota(jnp.int32, (pair_rows, dim), 0) < heads
    pairs = CHUNK // 2
    scale = dim ** -0.5
    per = per_group // CHUNK
    block = dim // rows

    def attend(i, _):
        rd(i, k_in, k_vm, ksem).wait()
        rd(i, v_in, v_vm, vsem).wait()

        @pl.when(i + DEPTH < chunks)
        def _():
            rd(i + DEPTH, k_in, k_vm, ksem).start()
            rd(i + DEPTH, v_in, v_vm, vsem).start()

        base = i * CHUNK
        grp = i // per
        tiles = []
        for j in range(CHUNK):
            slot = lens[base + j] - first
            start = pl.multiple_of((jnp.clip(slot, 0, pos - 1) // 16) * 16, 16)
            hit = tile_row + start == slot
            new = kv_scr[pl.ds(base + j, 1), :]
            kt = k_vm[base + j, pl.ds(start, 16), :].astype(F32)
            vt = v_vm[base + j, pl.ds(start, 16), :].astype(F32)
            tiles.append((start, jnp.where(hit, new[:, :dim], kt).astype(BF16),
                          jnp.where(hit, new[:, dim:], vt).astype(BF16)))
        for j, (start, kt, vt) in enumerate(tiles):
            k_vm[base + j, pl.ds(start, 16), :] = kt
            v_vm[base + j, pl.ds(start, 16), :] = vt
        wr(i, k_vm, k_out, kosem).start()
        wr(i, v_vm, v_out, vosem).start()
        scores = []
        for p in range(pairs):
            b = base + 2 * p
            keys = jnp.concatenate([k_vm[b], k_vm[b + 1]], axis=1)
            q = qd[i * pairs + p].astype(BF16)
            scores.append(lax.dot_general(q, keys, (((1,), (1,)), ((), ())), preferred_element_type=F32) * scale)
        weights = []
        for p in range(pairs):
            b = base + 2 * p
            valid = at <= jnp.where(row < heads, lens[b], lens[b + 1])
            sc = jnp.where(valid, scores[p], LOW)
            m = jnp.max(sc, axis=-1, keepdims=True)
            w = jnp.where(valid, jnp.exp(sc - m), 0.0)
            weights.append((m, jnp.sum(w, axis=-1, keepdims=True), w.astype(BF16)))
        for p in range(pairs):
            b = base + 2 * p
            m, total, w = weights[p]
            vals = jnp.concatenate([v_vm[b], v_vm[b + 1]], axis=1)
            o = jnp.dot(w, vals, preferred_element_type=F32)
            j = lax.rem(b, per_group)
            msg[grp, j // own, pl.ds(pl.multiple_of(lax.rem(j, own) * heads, pair_rows), pair_rows), :] = jnp.where(low_half, o[:, :dim], o[:, dim:])
            stat[pl.ds(pl.multiple_of(j * heads, pair_rows), pair_rows), :] = jnp.where(lane == 0, m, total)
        return 0

    for g in range(GROUPS):
        lax.fori_loop(g * per, (g + 1) * per, attend, 0)
        for a in range(n_sq // block):
            tile = stat[a * dim:(a + 1) * dim, :].T[0:8, :]
            for k in range(block):
                msg[g, a * block + k, rows:rows + 8, :] = tile
    for i in range(chunks):
        wr(i, k_vm, k_out, kosem).wait()
        wr(i, v_vm, v_out, vosem).wait()


def merge_kernel(n_tp, n_sq, heads, msg, wo, y_out, got1, mid, got2, fac, att, part, got3,
                 s1, r1, s2, r2, s3, r3, s4a, r4a, s4b, r4b, s4c, r4c):
    dim = msg.shape[-1]
    own, width = part.shape[1:]
    rows = own * heads
    cols = width // n_tp
    n_x = n_sq // 2
    block = dim // rows
    s = lax.axis_index("sq")
    t = lax.axis_index("tp")
    x, c = s // 2, lax.rem(s, 2)
    partner = {"sq": s + 1 - 2 * c}

    def x_peer(i):
        return {"sq": lax.rem(x + i, n_x) * 2 + c}

    def y_peer(i):
        return {"tp": lax.rem(t + i, n_tp)}

    def remote(src, dst, send, recv, to):
        return pltpu.make_async_remote_copy(src, dst, send, recv, device_id=to, device_id_type=MESH)

    def lanes(k, n):
        return pl.ds(pl.multiple_of(k * n, n), n)

    barrier = pltpu.get_barrier_semaphore()
    pl.semaphore_signal(barrier, inc=1, device_id=partner, device_id_type=MESH)
    for i in range(1, n_x):
        pl.semaphore_signal(barrier, inc=1, device_id=x_peer(i), device_id_type=MESH)
    for i in range(1, n_tp):
        pl.semaphore_signal(barrier, inc=1, device_id=y_peer(i), device_id_type=MESH)
    pl.semaphore_wait(barrier, n_x + n_tp - 1)

    def copy1(g):
        return remote(msg.at[g, :, 1 - c], got1.at[g], s1.at[g], r1.at[g], partner)

    def copy2(g, i):
        return remote(mid.at[g, lax.rem(x + i, n_x)], got2.at[g, i], s2.at[g, i], r2.at[g, i], x_peer(i))

    def copy3(g, i):
        return remote(part.at[g, :, lanes(lax.rem(t + i, n_tp), cols)], got3.at[g, i], s3.at[g, i], r3.at[g, i], y_peer(i))

    def dims(g):
        return (n_x, n_tp) if g % 2 == 0 else (n_tp, n_x)

    def peer(g, second, i):
        return y_peer(i) if (g % 2 == 0) == second else x_peer(i)

    def cell(g, a, b):
        dx, dt = (a, b) if g % 2 == 0 else (b, a)
        return y_out.at[g, lax.rem(x + n_x - dx, n_x), c, :, lanes(lax.rem(t + n_tp - dt, n_tp), cols)]

    def copy4a(g, i, back=0):
        return remote(cell(g, back, 0), cell(g, back, 0), s4a.at[g, i], r4a.at[g, i], peer(g, False, i))

    def copy4b(g, a, i, back=0):
        return remote(cell(g, a, back), cell(g, a, back), s4b.at[g, a, i], r4b.at[g, a, i], peer(g, True, i))

    def copy4c(g, i, core):
        if g % 2 == 0:
            ref = y_out.at[g, :, core, :, lanes(lax.rem(t + n_tp - i, n_tp), cols)]
        else:
            ref = y_out.at[g, lax.rem(x + n_x - i, n_x), core]
        return remote(ref, ref, s4c.at[g, i], r4c.at[g, i], partner)

    def merge1(g):
        copy1(g).wait_recv()
        fs, tiles = [], []
        for k in range(n_x):
            a, b = msg[g, k, c, rows:rows + 8, :], got1[g, k, rows:rows + 8, :]
            top = jnp.maximum(a[0:1], b[0:1])
            fa, fb = jnp.exp(a[0:1] - top), jnp.exp(b[0:1] - top)
            fs += [fa, fb]
            mid[g, k, rows:rows + 8, :] = jnp.concatenate([top, fa * a[1:2] + fb * b[1:2], jnp.zeros((6, dim), F32)], axis=0)
        f = jnp.concatenate(fs + [jnp.zeros((dim - 2 * n_x, dim), F32)], axis=0)
        fac[...] = f.T
        for k in range(n_x):
            fcol = fac[lanes(lax.rem(2 * k + c, block), rows), :]
            mid[g, k, 0:rows, :] = msg[g, k, c, 0:rows, :] * fcol[:, 2 * k:2 * k + 1] + got1[g, k, 0:rows, :] * fcol[:, 2 * k + 1:2 * k + 2]
        for i in range(1, n_x):
            copy2(g, i).start()

    def merge2(g):
        for i in range(1, n_x):
            copy2(g, i).wait_recv()
        tiles = [mid[g, x, rows:rows + 8, :]] + [got2[g, i, rows:rows + 8, :] for i in range(1, n_x)]
        m = jnp.concatenate([v[0:1] for v in tiles], axis=0)
        total = jnp.concatenate([v[1:2] for v in tiles], axis=0)
        f = jnp.exp(m - jnp.max(m, axis=0, keepdims=True))
        f = f / jnp.sum(f * total, axis=0, keepdims=True)
        fac[...] = jnp.concatenate([f, jnp.zeros((dim - n_x, dim), F32)], axis=0).T
        fcol = fac[lanes(lax.rem(s, block), rows), :]
        a = mid[g, x, 0:rows, :] * fcol[:, 0:1]
        for i in range(1, n_x):
            a = a + got2[g, i, 0:rows, :] * fcol[:, i:i + 1]
        att[...] = a
        lhs = jnp.concatenate([att[pl.ds(h, own, stride=heads), :] for h in range(heads)], axis=1).astype(BF16)
        part[g] = jnp.dot(lhs, wo[...], preferred_element_type=F32)
        for i in range(1, n_tp):
            copy3(g, i).start()

    def reduce3(g):
        for i in range(1, n_tp):
            copy3(g, i).wait_recv()
        y = part[g, :, lanes(t, cols)]
        for i in range(1, n_tp):
            y = y + got3[g, i]
        y_out[g, x, c, :, lanes(t, cols)] = y
        na, nb = dims(g)
        for i in range(1, na):
            copy4a(g, i).start()
        for i in range(1, nb):
            copy4b(g, 0, i).start()

    def nearest(n):
        return sorted(range(1, n), key=lambda i: min(i, n - i))

    def forward4(g):
        na, nb = dims(g)
        for a in nearest(na):
            copy4a(g, a, a).wait_recv()
            for i in range(1, nb):
                copy4b(g, a, i).start()
        copy4c(g, 0, c).start()

    def collect4(g):
        na, nb = dims(g)
        for i in nearest(nb):
            for a in range(na):
                copy4b(g, a, i, i).wait_recv()
            copy4c(g, i, c).start()

    for g in range(GROUPS):
        copy1(g).start()
    for g in range(GROUPS):
        merge1(g)
    stages = (merge2, reduce3, forward4, collect4)
    for step in range(GROUPS + len(stages) - 1):
        for k, stage in enumerate(stages):
            if 0 <= step - k < GROUPS:
                stage(step - k)
    for g in range(GROUPS):
        na, nb = dims(g)
        for i in range(nb):
            copy4c(g, i, 1 - c).wait_recv()
    for g in range(GROUPS):
        na, nb = dims(g)
        copy1(g).wait_send()
        for i in range(1, n_x):
            copy2(g, i).wait_send()
        for i in range(1, n_tp):
            copy3(g, i).wait_send()
        for i in range(1, na):
            copy4a(g, i).wait_send()
        for a in range(na):
            for i in range(1, nb):
                copy4b(g, a, i).wait_send()
        for i in range(nb):
            copy4c(g, i, c).wait_send()


VM = pl.BlockSpec(memory_space=pltpu.VMEM)
SM = pl.BlockSpec(memory_space=pltpu.SMEM)
ANYW = pl.BlockSpec(memory_space=pl.ANY)
DMA = pltpu.SemaphoreType.DMA


def attend(n_sq, cache_lens, hidden, ln_gain, ln_bias, w_query, b_query, w_kv, b_kv, k_cache, v_cache):
    batch, pos, dim = k_cache.shape
    heads = w_query.shape[1] // dim
    chunks = batch // CHUNK
    rows = batch // GROUPS // n_sq * heads
    return pl.pallas_call(
        functools.partial(attend_kernel, n_sq),
        in_specs=[SM, ANYW, VM, VM, ANYW, VM, ANYW, VM, ANYW, ANYW],
        out_specs=[ANYW, ANYW, VM],
        out_shape=[jax.ShapeDtypeStruct(k_cache.shape, BF16), jax.ShapeDtypeStruct(v_cache.shape, BF16),
                   pltpu.VMEM((GROUPS, n_sq, rows + 8, dim), F32)],
        scratch_shapes=[
            pltpu.VMEM(hidden.shape, BF16), pltpu.VMEM(w_query.shape, BF16), pltpu.VMEM(w_kv.shape, BF16),
            pltpu.VMEM(hidden.shape, BF16), pltpu.VMEM((batch, 2 * dim), F32),
            pltpu.VMEM((batch // 2, 2 * heads, 2 * dim), F32),
            pltpu.VMEM((batch // GROUPS * heads, dim), F32),
            pltpu.VMEM(k_cache.shape, BF16), pltpu.VMEM(v_cache.shape, BF16),
            DMA((3,)), *[DMA((chunks,)) for _ in range(4)],
        ],
        compiler_params=pltpu.CompilerParams(vmem_limit_bytes=54 << 20),
        cost_estimate=pl.CostEstimate(flops=4 * batch * pos * dim * heads * 2, bytes_accessed=4 * k_cache.size, transcendentals=0),
        name="attend",
    )(cache_lens, hidden, ln_gain.reshape(1, -1), ln_bias.reshape(1, -1), w_query, b_query.reshape(1, -1),
      w_kv, b_kv.reshape(1, -1), k_cache, v_cache)


def merge(n_tp, n_sq, batch, heads, msg, w_out):
    dim = msg.shape[-1]
    width = w_out.shape[1]
    own = batch // GROUPS // n_sq
    cols = width // n_tp
    n_x = n_sq // 2
    most = max(n_tp, n_x)
    shapes = [(GROUPS,), (GROUPS, n_x), (GROUPS, n_tp), (GROUPS, most), (GROUPS, most, most), (GROUPS, most)]
    return pl.pallas_call(
        functools.partial(merge_kernel, n_tp, n_sq, heads),
        in_specs=[VM, VM],
        out_specs=VM,
        out_shape=pltpu.VMEM((GROUPS, n_x, 2, own, width), F32),
        scratch_shapes=[
            *[pltpu.VMEM((GROUPS, n_x, *msg.shape[2:]), F32) for _ in range(3)],
            pltpu.VMEM((dim, dim), F32), pltpu.VMEM((own * heads, dim), F32),
            pltpu.VMEM((GROUPS, own, width), F32), pltpu.VMEM((GROUPS, n_tp, own, cols), F32),
            *[DMA(shape) for shape in shapes for _ in range(2)],
        ],
        compiler_params=pltpu.CompilerParams(collective_id=0, has_side_effects=True, vmem_limit_bytes=8 << 20),
        cost_estimate=pl.CostEstimate(flops=40 * batch * 256 * dim * heads, bytes_accessed=4 * batch * width, transcendentals=0),
        name="merge",
    )(msg.reshape(GROUPS, n_x, 2, *msg.shape[2:]), w_out)


def solution(mesh):
    n_tp, n_sq = mesh.shape["tp"], mesh.shape["sq"]

    def local_step(hidden, cache_lens, k_cache, v_cache, ln_gain, ln_bias, w_query, b_query, w_kv, b_kv, w_out, b_out):
        batch, pos, dim = k_cache.shape
        heads = w_query.shape[1] // dim
        key_new, val_new, msg = attend(n_sq, cache_lens, hidden, ln_gain, ln_bias, w_query, b_query, w_kv, b_kv, k_cache, v_cache)
        y = merge(n_tp, n_sq, batch, heads, msg, w_out)
        out_hidden = (hidden.astype(F32) + y.reshape(hidden.shape) + b_out).astype(BF16)
        return out_hidden, key_new, val_new

    cache_spec = P("dp", "sq", None)
    row_spec = P("dp", None)
    in_specs = (row_spec, P("dp"), cache_spec, cache_spec, P(None), P(None), P(None, "tp"), P("tp"), P(None, None), P(None), P("tp", None), P(None))
    return jax.shard_map(local_step, mesh=mesh, in_specs=in_specs, out_specs=(row_spec, cache_spec, cache_spec), check_vma=False)
```

```python
import functools
import jax
import jax.numpy as jnp
from jax import lax
from jax.sharding import PartitionSpec as P
from jax.experimental import pallas as pl
from jax.experimental.pallas import tpu as pltpu

F32 = jnp.float32
BF16 = jnp.bfloat16
MESH = pl.DeviceIdType.MESH
CHUNK = 16
DEPTH = 8
EARLY = 3
GROUPS = 2
LOW = -1e30


def attend_kernel(n_sq, lens, hid_h, gain, bias, wq_h, bq, wkv_h, bkv, k_in, v_in,
                  k_out, v_out, msg,
                  hid, wq, wkv, h_scr, kv_scr, qd, stat, k_vm, v_vm, wsem, ksem, vsem, kosem, vosem):
    batch, pos, dim = k_in.shape
    heads = wq.shape[1] // dim
    chunks = batch // CHUNK
    per_group = batch // GROUPS
    own = per_group // n_sq
    rows = own * heads
    first = lax.axis_index("sq") * pos

    wcopies = [pltpu.make_async_copy(src, dst, wsem.at[i])
               for i, (src, dst) in enumerate(((hid_h, hid), (wkv_h, wkv), (wq_h, wq)))]

    def rd(i, src, buf, sem):
        span = pl.ds(i * CHUNK, CHUNK)
        return pltpu.make_async_copy(src.at[span], buf.at[span], sem.at[i])

    def wr(i, buf, dst, sem):
        span = pl.ds(i * CHUNK, CHUNK)
        return pltpu.make_async_copy(buf.at[span], dst.at[span], sem.at[i])

    for copy in wcopies:
        copy.start()

    wcopies[0].wait()
    for i in range(EARLY):
        rd(i, k_in, k_vm, ksem).start()
        rd(i, v_in, v_vm, vsem).start()
    nrow = 32

    def norm_rows(i, _):
        span = pl.ds(pl.multiple_of(i * nrow, nrow), nrow)
        wide = hid[span, :].astype(F32)
        mean = jnp.mean(wide, axis=-1, keepdims=True)
        cent = wide - mean
        var = jnp.mean(cent * cent, axis=-1, keepdims=True)
        normed = cent * lax.rsqrt(var + 1e-5)
        h_scr[span, :] = (normed * gain[...] + bias[...]).astype(BF16)
        return 0

    lax.fori_loop(0, batch // nrow, norm_rows, 0)
    wcopies[1].wait()
    wcopies[2].wait()
    for i in range(EARLY, DEPTH):
        rd(i, k_in, k_vm, ksem).start()
        rd(i, v_in, v_vm, vsem).start()
    kv = jnp.dot(h_scr[...], wkv[...], preferred_element_type=F32) + bkv[...]
    kv_scr[...] = kv.astype(BF16).astype(F32)
    qd[...] = jnp.zeros_like(qd)
    for h in range(heads):
        span = slice(h * dim, (h + 1) * dim)
        q = jnp.dot(h_scr[...], wq[:, span], preferred_element_type=F32) + bq[:, span]
        q = q.astype(BF16).astype(F32).reshape(batch // 2, 2, dim)
        qd[:, h, 0:dim] = q[:, 0, :]
        qd[:, heads + h, dim:2 * dim] = q[:, 1, :]

    pair_rows = 2 * heads
    row = lax.broadcasted_iota(jnp.int32, (pair_rows, pos), 0)
    at = first + lax.broadcasted_iota(jnp.int32, (pair_rows, pos), 1)
    tile_row = lax.broadcasted_iota(jnp.int32, (16, dim), 0)
    lane = lax.broadcasted_iota(jnp.int32, (pair_rows, dim), 1)
    low_half = lax.broadcasted_iota(jnp.int32, (pair_rows, dim), 0) < heads
    pairs = CHUNK // 2
    scale = dim ** -0.5
    per = per_group // CHUNK
    block = dim // rows

    def attend(i, _):
        rd(i, k_in, k_vm, ksem).wait()
        rd(i, v_in, v_vm, vsem).wait()

        @pl.when(i + DEPTH < chunks)
        def _():
            rd(i + DEPTH, k_in, k_vm, ksem).start()
            rd(i + DEPTH, v_in, v_vm, vsem).start()

        base = i * CHUNK
        grp = i // per
        tiles = []
        for j in range(CHUNK):
            slot = lens[base + j] - first
            start = pl.multiple_of((jnp.clip(slot, 0, pos - 1) // 16) * 16, 16)
            hit = tile_row + start == slot
            new = kv_scr[pl.ds(base + j, 1), :]
            kt = k_vm[base + j, pl.ds(start, 16), :].astype(F32)
            vt = v_vm[base + j, pl.ds(start, 16), :].astype(F32)
            tiles.append((start, jnp.where(hit, new[:, :dim], kt).astype(BF16),
                          jnp.where(hit, new[:, dim:], vt).astype(BF16)))
        for j, (start, kt, vt) in enumerate(tiles):
            k_vm[base + j, pl.ds(start, 16), :] = kt
            v_vm[base + j, pl.ds(start, 16), :] = vt
        wr(i, k_vm, k_out, kosem).start()
        wr(i, v_vm, v_out, vosem).start()
        scores = []
        for p in range(pairs):
            b = base + 2 * p
            keys = jnp.concatenate([k_vm[b], k_vm[b + 1]], axis=1)
            q = qd[i * pairs + p].astype(BF16)
            scores.append(lax.dot_general(q, keys, (((1,), (1,)), ((), ())), preferred_element_type=F32) * scale)
        weights = []
        for p in range(pairs):
            b = base + 2 * p
            valid = at <= jnp.where(row < heads, lens[b], lens[b + 1])
            sc = jnp.where(valid, scores[p], LOW)
            m = jnp.max(sc, axis=-1, keepdims=True)
            w = jnp.where(valid, jnp.exp(sc - m), 0.0)
            weights.append((m, jnp.sum(w, axis=-1, keepdims=True), w.astype(BF16)))
        for p in range(pairs):
            b = base + 2 * p
            m, total, w = weights[p]
            vals = jnp.concatenate([v_vm[b], v_vm[b + 1]], axis=1)
            o = jnp.dot(w, vals, preferred_element_type=F32)
            j = lax.rem(b, per_group)
            msg[grp, j // own, pl.ds(pl.multiple_of(lax.rem(j, own) * heads, pair_rows), pair_rows), :] = jnp.where(low_half, o[:, :dim], o[:, dim:])
            stat[pl.ds(pl.multiple_of(j * heads, pair_rows), pair_rows), :] = jnp.where(lane == 0, m, total)
        return 0

    for g in range(GROUPS):
        lax.fori_loop(g * per, (g + 1) * per, attend, 0)
        for a in range(n_sq // block):
            tile = stat[a * dim:(a + 1) * dim, :].T[0:8, :]
            for k in range(block):
                msg[g, a * block + k, rows:rows + 8, :] = tile
    for i in range(chunks):
        wr(i, k_vm, k_out, kosem).wait()
        wr(i, v_vm, v_out, vosem).wait()


def merge_kernel(n_tp, n_sq, heads, msg, wo, y_out, got1, mid, got2, fac, att, part, got3,
                 s1, r1, s2, r2, s3, r3, s4a, r4a, s4b, r4b, s4c, r4c):
    dim = msg.shape[-1]
    own, width = part.shape[1:]
    rows = own * heads
    cols = width // n_tp
    n_x = n_sq // 2
    block = dim // rows
    s = lax.axis_index("sq")
    t = lax.axis_index("tp")
    x, c = s // 2, lax.rem(s, 2)
    partner = {"sq": s + 1 - 2 * c}

    def x_peer(i):
        return {"sq": lax.rem(x + i, n_x) * 2 + c}

    def y_peer(i):
        return {"tp": lax.rem(t + i, n_tp)}

    def remote(src, dst, send, recv, to):
        return pltpu.make_async_remote_copy(src, dst, send, recv, device_id=to, device_id_type=MESH)

    def lanes(k, n):
        return pl.ds(pl.multiple_of(k * n, n), n)

    barrier = pltpu.get_barrier_semaphore()
    pl.semaphore_signal(barrier, inc=1, device_id=partner, device_id_type=MESH)
    for i in range(1, n_x):
        pl.semaphore_signal(barrier, inc=1, device_id=x_peer(i), device_id_type=MESH)
    for i in range(1, n_tp):
        pl.semaphore_signal(barrier, inc=1, device_id=y_peer(i), device_id_type=MESH)
    pl.semaphore_wait(barrier, n_x + n_tp - 1)

    def copy1(g):
        return remote(msg.at[g, :, 1 - c], got1.at[g], s1.at[g], r1.at[g], partner)

    def copy2(g, i):
        return remote(mid.at[g, lax.rem(x + i, n_x)], got2.at[g, i], s2.at[g, i], r2.at[g, i], x_peer(i))

    def copy3(g, i):
        return remote(part.at[g, :, lanes(lax.rem(t + i, n_tp), cols)], got3.at[g, i], s3.at[g, i], r3.at[g, i], y_peer(i))

    def dims(g):
        return (n_x, n_tp) if g % 2 == 0 else (n_tp, n_x)

    def peer(g, second, i):
        return y_peer(i) if (g % 2 == 0) == second else x_peer(i)

    def cell(g, a, b):
        dx, dt = (a, b) if g % 2 == 0 else (b, a)
        return y_out.at[g, lax.rem(x + n_x - dx, n_x), c, :, lanes(lax.rem(t + n_tp - dt, n_tp), cols)]

    def copy4a(g, i, back=0):
        return remote(cell(g, back, 0), cell(g, back, 0), s4a.at[g, i], r4a.at[g, i], peer(g, False, i))

    def copy4b(g, a, i, back=0):
        return remote(cell(g, a, back), cell(g, a, back), s4b.at[g, a, i], r4b.at[g, a, i], peer(g, True, i))

    def copy4c(g, i, core):
        if g % 2 == 0:
            ref = y_out.at[g, :, core, :, lanes(lax.rem(t + n_tp - i, n_tp), cols)]
        else:
            ref = y_out.at[g, lax.rem(x + n_x - i, n_x), core]
        return remote(ref, ref, s4c.at[g, i], r4c.at[g, i], partner)

    def merge1(g):
        copy1(g).wait_recv()
        fs, tiles = [], []
        for k in range(n_x):
            a, b = msg[g, k, c, rows:rows + 8, :], got1[g, k, rows:rows + 8, :]
            top = jnp.maximum(a[0:1], b[0:1])
            fa, fb = jnp.exp(a[0:1] - top), jnp.exp(b[0:1] - top)
            fs += [fa, fb]
            mid[g, k, rows:rows + 8, :] = jnp.concatenate([top, fa * a[1:2] + fb * b[1:2], jnp.zeros((6, dim), F32)], axis=0)
        f = jnp.concatenate(fs + [jnp.zeros((dim - 2 * n_x, dim), F32)], axis=0)
        fac[...] = f.T
        for k in range(n_x):
            fcol = fac[lanes(lax.rem(2 * k + c, block), rows), :]
            mid[g, k, 0:rows, :] = msg[g, k, c, 0:rows, :] * fcol[:, 2 * k:2 * k + 1] + got1[g, k, 0:rows, :] * fcol[:, 2 * k + 1:2 * k + 2]
        for i in range(1, n_x):
            copy2(g, i).start()

    def merge2(g):
        for i in range(1, n_x):
            copy2(g, i).wait_recv()
        tiles = [mid[g, x, rows:rows + 8, :]] + [got2[g, i, rows:rows + 8, :] for i in range(1, n_x)]
        m = jnp.concatenate([v[0:1] for v in tiles], axis=0)
        total = jnp.concatenate([v[1:2] for v in tiles], axis=0)
        f = jnp.exp(m - jnp.max(m, axis=0, keepdims=True))
        f = f / jnp.sum(f * total, axis=0, keepdims=True)
        fac[...] = jnp.concatenate([f, jnp.zeros((dim - n_x, dim), F32)], axis=0).T
        fcol = fac[lanes(lax.rem(s, block), rows), :]
        a = mid[g, x, 0:rows, :] * fcol[:, 0:1]
        for i in range(1, n_x):
            a = a + got2[g, i, 0:rows, :] * fcol[:, i:i + 1]
        att[...] = a
        lhs = jnp.concatenate([att[pl.ds(h, own, stride=heads), :] for h in range(heads)], axis=1).astype(BF16)
        part[g] = jnp.dot(lhs, wo[...], preferred_element_type=F32)
        for i in range(1, n_tp):
            copy3(g, i).start()

    def reduce3(g):
        for i in range(1, n_tp):
            copy3(g, i).wait_recv()
        y = part[g, :, lanes(t, cols)]
        for i in range(1, n_tp):
            y = y + got3[g, i]
        y_out[g, x, c, :, lanes(t, cols)] = y
        na, nb = dims(g)
        for i in range(1, na):
            copy4a(g, i).start()
        for i in range(1, nb):
            copy4b(g, 0, i).start()

    def nearest(n):
        return sorted(range(1, n), key=lambda i: min(i, n - i))

    def forward4(g):
        na, nb = dims(g)
        for a in nearest(na):
            copy4a(g, a, a).wait_recv()
            for i in range(1, nb):
                copy4b(g, a, i).start()
        copy4c(g, 0, c).start()

    def collect4(g):
        na, nb = dims(g)
        for i in nearest(nb):
            for a in range(na):
                copy4b(g, a, i, i).wait_recv()
            copy4c(g, i, c).start()

    for g in range(GROUPS):
        copy1(g).start()
    for g in range(GROUPS):
        merge1(g)
    stages = (merge2, reduce3, forward4, collect4)
    for step in range(GROUPS + len(stages) - 1):
        for k, stage in enumerate(stages):
            if 0 <= step - k < GROUPS:
                stage(step - k)
    for g in range(GROUPS):
        na, nb = dims(g)
        for i in range(nb):
            copy4c(g, i, 1 - c).wait_recv()
    for g in range(GROUPS):
        na, nb = dims(g)
        copy1(g).wait_send()
        for i in range(1, n_x):
            copy2(g, i).wait_send()
        for i in range(1, n_tp):
            copy3(g, i).wait_send()
        for i in range(1, na):
            copy4a(g, i).wait_send()
        for a in range(na):
            for i in range(1, nb):
                copy4b(g, a, i).wait_send()
        for i in range(nb):
            copy4c(g, i, c).wait_send()


VM = pl.BlockSpec(memory_space=pltpu.VMEM)
SM = pl.BlockSpec(memory_space=pltpu.SMEM)
ANYW = pl.BlockSpec(memory_space=pl.ANY)
DMA = pltpu.SemaphoreType.DMA


def attend(n_sq, cache_lens, hidden, ln_gain, ln_bias, w_query, b_query, w_kv, b_kv, k_cache, v_cache):
    batch, pos, dim = k_cache.shape
    heads = w_query.shape[1] // dim
    chunks = batch // CHUNK
    rows = batch // GROUPS // n_sq * heads
    return pl.pallas_call(
        functools.partial(attend_kernel, n_sq),
        in_specs=[SM, ANYW, VM, VM, ANYW, VM, ANYW, VM, ANYW, ANYW],
        out_specs=[ANYW, ANYW, VM],
        out_shape=[jax.ShapeDtypeStruct(k_cache.shape, BF16), jax.ShapeDtypeStruct(v_cache.shape, BF16),
                   pltpu.VMEM((GROUPS, n_sq, rows + 8, dim), F32)],
        scratch_shapes=[
            pltpu.VMEM(hidden.shape, BF16), pltpu.VMEM(w_query.shape, BF16), pltpu.VMEM(w_kv.shape, BF16),
            pltpu.VMEM(hidden.shape, BF16), pltpu.VMEM((batch, 2 * dim), F32),
            pltpu.VMEM((batch // 2, 2 * heads, 2 * dim), F32),
            pltpu.VMEM((batch // GROUPS * heads, dim), F32),
            pltpu.VMEM(k_cache.shape, BF16), pltpu.VMEM(v_cache.shape, BF16),
            DMA((3,)), *[DMA((chunks,)) for _ in range(4)],
        ],
        compiler_params=pltpu.CompilerParams(vmem_limit_bytes=54 << 20),
        cost_estimate=pl.CostEstimate(flops=4 * batch * pos * dim * heads * 2, bytes_accessed=4 * k_cache.size, transcendentals=0),
        name="attend",
    )(cache_lens, hidden, ln_gain.reshape(1, -1), ln_bias.reshape(1, -1), w_query, b_query.reshape(1, -1),
      w_kv, b_kv.reshape(1, -1), k_cache, v_cache)


def merge(n_tp, n_sq, batch, heads, msg, w_out):
    dim = msg.shape[-1]
    width = w_out.shape[1]
    own = batch // GROUPS // n_sq
    cols = width // n_tp
    n_x = n_sq // 2
    most = max(n_tp, n_x)
    shapes = [(GROUPS,), (GROUPS, n_x), (GROUPS, n_tp), (GROUPS, most), (GROUPS, most, most), (GROUPS, most)]
    return pl.pallas_call(
        functools.partial(merge_kernel, n_tp, n_sq, heads),
        in_specs=[VM, VM],
        out_specs=VM,
        out_shape=pltpu.VMEM((GROUPS, n_x, 2, own, width), F32),
        scratch_shapes=[
            *[pltpu.VMEM((GROUPS, n_x, *msg.shape[2:]), F32) for _ in range(3)],
            pltpu.VMEM((dim, dim), F32), pltpu.VMEM((own * heads, dim), F32),
            pltpu.VMEM((GROUPS, own, width), F32), pltpu.VMEM((GROUPS, n_tp, own, cols), F32),
            *[DMA(shape) for shape in shapes for _ in range(2)],
        ],
        compiler_params=pltpu.CompilerParams(collective_id=0, has_side_effects=True, vmem_limit_bytes=8 << 20),
        cost_estimate=pl.CostEstimate(flops=40 * batch * 256 * dim * heads, bytes_accessed=4 * batch * width, transcendentals=0),
        name="merge",
    )(msg.reshape(GROUPS, n_x, 2, *msg.shape[2:]), w_out)


def solution(mesh):
    n_tp, n_sq = mesh.shape["tp"], mesh.shape["sq"]

    def local_step(hidden, cache_lens, k_cache, v_cache, ln_gain, ln_bias, w_query, b_query, w_kv, b_kv, w_out, b_out):
        batch, pos, dim = k_cache.shape
        heads = w_query.shape[1] // dim
        key_new, val_new, msg = attend(n_sq, cache_lens, hidden, ln_gain, ln_bias, w_query, b_query, w_kv, b_kv, k_cache, v_cache)
        y = merge(n_tp, n_sq, batch, heads, msg, w_out)
        out_hidden = (hidden.astype(F32) + y.reshape(hidden.shape) + b_out).astype(BF16)
        return out_hidden, key_new, val_new

    cache_spec = P("dp", "sq", None)
    row_spec = P("dp", None)
    in_specs = (row_spec, P("dp"), cache_spec, cache_spec, P(None), P(None), P(None, "tp"), P("tp"), P(None, None), P(None), P("tp", None), P(None))
    return jax.shard_map(local_step, mesh=mesh, in_specs=in_specs, out_specs=(row_spec, cache_spec, cache_spec), check_vma=False)
```

```python
import functools
import jax
import jax.numpy as jnp
from jax import lax
from jax.sharding import PartitionSpec as P
from jax.experimental import pallas as pl
from jax.experimental.pallas import tpu as pltpu

F32 = jnp.float32
BF16 = jnp.bfloat16
MESH = pl.DeviceIdType.MESH
CHUNK = 16
DEPTH = 8
EARLY = 3
GROUPS = 2
LOW = float(jnp.finfo(F32).min)


def attend_kernel(n_sq, lens, hid_h, gain, bias, wq_h, bq, wkv_h, bkv, k_in, v_in,
                  k_out, v_out, msg,
                  hid, wq, wkv, h_scr, kv_scr, qd, stat, k_vm, v_vm, wsem, ksem, vsem, kosem, vosem):
    batch, pos, dim = k_in.shape
    heads = wq.shape[1] // dim
    chunks = batch // CHUNK
    per_group = batch // GROUPS
    own = per_group // n_sq
    rows = own * heads
    first = lax.axis_index("sq") * pos

    wcopies = [pltpu.make_async_copy(src, dst, wsem.at[i])
               for i, (src, dst) in enumerate(((hid_h, hid), (wkv_h, wkv), (wq_h, wq)))]

    def rd(i, src, buf, sem):
        span = pl.ds(i * CHUNK, CHUNK)
        return pltpu.make_async_copy(src.at[span], buf.at[span], sem.at[i])

    def wr(i, buf, dst, sem):
        span = pl.ds(i * CHUNK, CHUNK)
        return pltpu.make_async_copy(buf.at[span], dst.at[span], sem.at[i])

    for copy in wcopies:
        copy.start()

    wcopies[0].wait()
    for i in range(EARLY):
        rd(i, k_in, k_vm, ksem).start()
        rd(i, v_in, v_vm, vsem).start()
    nrow = 32

    def norm_rows(i, _):
        span = pl.ds(pl.multiple_of(i * nrow, nrow), nrow)
        wide = hid[span, :].astype(F32)
        mean = jnp.mean(wide, axis=-1, keepdims=True)
        cent = wide - mean
        var = jnp.mean(cent * cent, axis=-1, keepdims=True)
        normed = cent * lax.rsqrt(var + 1e-5)
        h_scr[span, :] = (normed * gain[...] + bias[...]).astype(BF16)
        return 0

    lax.fori_loop(0, batch // nrow, norm_rows, 0)
    wcopies[1].wait()
    wcopies[2].wait()
    for i in range(EARLY, DEPTH):
        rd(i, k_in, k_vm, ksem).start()
        rd(i, v_in, v_vm, vsem).start()
    kv = jnp.dot(h_scr[...], wkv[...], preferred_element_type=F32) + bkv[...]
    kv_scr[...] = kv.astype(BF16).astype(F32)
    qd[...] = jnp.zeros_like(qd)
    for h in range(heads):
        span = slice(h * dim, (h + 1) * dim)
        q = jnp.dot(h_scr[...], wq[:, span], preferred_element_type=F32) + bq[:, span]
        q = q.astype(BF16).astype(F32).reshape(batch // 2, 2, dim)
        qd[:, h, 0:dim] = q[:, 0, :]
        qd[:, heads + h, dim:2 * dim] = q[:, 1, :]

    pair_rows = 2 * heads
    row = lax.broadcasted_iota(jnp.int32, (pair_rows, pos), 0)
    at = first + lax.broadcasted_iota(jnp.int32, (pair_rows, pos), 1)
    tile_row = lax.broadcasted_iota(jnp.int32, (16, dim), 0)
    lane = lax.broadcasted_iota(jnp.int32, (pair_rows, dim), 1)
    low_half = lax.broadcasted_iota(jnp.int32, (pair_rows, dim), 0) < heads
    pairs = CHUNK // 2
    scale = dim ** -0.5
    per = per_group // CHUNK
    block = dim // rows

    def attend(i, _):
        rd(i, k_in, k_vm, ksem).wait()
        rd(i, v_in, v_vm, vsem).wait()

        @pl.when(i + DEPTH < chunks)
        def _():
            rd(i + DEPTH, k_in, k_vm, ksem).start()
            rd(i + DEPTH, v_in, v_vm, vsem).start()

        base = i * CHUNK
        grp = i // per
        tiles = []
        for j in range(CHUNK):
            slot = lens[base + j] - first
            start = pl.multiple_of((jnp.clip(slot, 0, pos - 1) // 16) * 16, 16)
            hit = tile_row + start == slot
            new = kv_scr[pl.ds(base + j, 1), :]
            kt = k_vm[base + j, pl.ds(start, 16), :].astype(F32)
            vt = v_vm[base + j, pl.ds(start, 16), :].astype(F32)
            tiles.append((start, jnp.where(hit, new[:, :dim], kt).astype(BF16),
                          jnp.where(hit, new[:, dim:], vt).astype(BF16)))
        for j, (start, kt, vt) in enumerate(tiles):
            k_vm[base + j, pl.ds(start, 16), :] = kt
            v_vm[base + j, pl.ds(start, 16), :] = vt
        wr(i, k_vm, k_out, kosem).start()
        wr(i, v_vm, v_out, vosem).start()
        scores = []
        for p in range(pairs):
            b = base + 2 * p
            keys = jnp.concatenate([k_vm[b], k_vm[b + 1]], axis=1)
            q = qd[i * pairs + p].astype(BF16)
            scores.append(lax.dot_general(q, keys, (((1,), (1,)), ((), ())), preferred_element_type=F32) * scale)
        weights = []
        for p in range(pairs):
            b = base + 2 * p
            valid = at <= jnp.where(row < heads, lens[b], lens[b + 1])
            sc = jnp.where(valid, scores[p], LOW)
            m = jnp.max(sc, axis=-1, keepdims=True)
            w = jnp.where(valid, jnp.exp(sc - m), 0.0)
            weights.append((m, jnp.sum(w, axis=-1, keepdims=True), w.astype(BF16)))
        for p in range(pairs):
            b = base + 2 * p
            m, total, w = weights[p]
            vals = jnp.concatenate([v_vm[b], v_vm[b + 1]], axis=1)
            o = jnp.dot(w, vals, preferred_element_type=F32)
            j = lax.rem(b, per_group)
            msg[grp, j // own, pl.ds(pl.multiple_of(lax.rem(j, own) * heads, pair_rows), pair_rows), :] = jnp.where(low_half, o[:, :dim], o[:, dim:])
            stat[pl.ds(pl.multiple_of(j * heads, pair_rows), pair_rows), :] = jnp.where(lane == 0, m, total)
        return 0

    for g in range(GROUPS):
        lax.fori_loop(g * per, (g + 1) * per, attend, 0)
        for a in range(n_sq // block):
            tile = stat[a * dim:(a + 1) * dim, :].T[0:8, :]
            for k in range(block):
                msg[g, a * block + k, rows:rows + 8, :] = tile
    for i in range(chunks):
        wr(i, k_vm, k_out, kosem).wait()
        wr(i, v_vm, v_out, vosem).wait()


def merge_kernel(n_tp, n_sq, heads, msg, wo, y_out, got1, mid, got2, fac, att, part, got3,
                 s1, r1, s2, r2, s3, r3, s4a, r4a, s4b, r4b, s4c, r4c):
    dim = msg.shape[-1]
    own, width = part.shape[1:]
    rows = own * heads
    cols = width // n_tp
    n_x = n_sq // 2
    block = dim // rows
    s = lax.axis_index("sq")
    t = lax.axis_index("tp")
    x, c = s // 2, lax.rem(s, 2)
    partner = {"sq": s + 1 - 2 * c}

    def x_peer(i):
        return {"sq": lax.rem(x + i, n_x) * 2 + c}

    def y_peer(i):
        return {"tp": lax.rem(t + i, n_tp)}

    def remote(src, dst, send, recv, to):
        return pltpu.make_async_remote_copy(src, dst, send, recv, device_id=to, device_id_type=MESH)

    def lanes(k, n):
        return pl.ds(pl.multiple_of(k * n, n), n)

    barrier = pltpu.get_barrier_semaphore()
    pl.semaphore_signal(barrier, inc=1, device_id=partner, device_id_type=MESH)
    for i in range(1, n_x):
        pl.semaphore_signal(barrier, inc=1, device_id=x_peer(i), device_id_type=MESH)
    for i in range(1, n_tp):
        pl.semaphore_signal(barrier, inc=1, device_id=y_peer(i), device_id_type=MESH)
    pl.semaphore_wait(barrier, n_x + n_tp - 1)

    def copy1(g):
        return remote(msg.at[g, :, 1 - c], got1.at[g], s1.at[g], r1.at[g], partner)

    def copy2(g, i):
        return remote(mid.at[g, lax.rem(x + i, n_x)], got2.at[g, i], s2.at[g, i], r2.at[g, i], x_peer(i))

    def copy3(g, i):
        return remote(part.at[g, :, lanes(lax.rem(t + i, n_tp), cols)], got3.at[g, i], s3.at[g, i], r3.at[g, i], y_peer(i))

    def dims(g):
        return (n_x, n_tp) if g % 2 == 1 else (n_tp, n_x)

    def peer(g, second, i):
        return y_peer(i) if (g % 2 == 1) == second else x_peer(i)

    def cell(g, a, b):
        dx, dt = (a, b) if g % 2 == 1 else (b, a)
        return y_out.at[g, lax.rem(x + n_x - dx, n_x), c, :, lanes(lax.rem(t + n_tp - dt, n_tp), cols)]

    def copy4a(g, i, back=0):
        return remote(cell(g, back, 0), cell(g, back, 0), s4a.at[g, i], r4a.at[g, i], peer(g, False, i))

    def copy4b(g, a, i, back=0):
        return remote(cell(g, a, back), cell(g, a, back), s4b.at[g, a, i], r4b.at[g, a, i], peer(g, True, i))

    def copy4c(g, i, core):
        if g % 2 == 1:
            ref = y_out.at[g, :, core, :, lanes(lax.rem(t + n_tp - i, n_tp), cols)]
        else:
            ref = y_out.at[g, lax.rem(x + n_x - i, n_x), core]
        return remote(ref, ref, s4c.at[g, i], r4c.at[g, i], partner)

    def merge1(g):
        copy1(g).wait_recv()
        fs, tiles = [], []
        for k in range(n_x):
            a, b = msg[g, k, c, rows:rows + 8, :], got1[g, k, rows:rows + 8, :]
            top = jnp.maximum(a[0:1], b[0:1])
            fa, fb = jnp.exp(a[0:1] - top), jnp.exp(b[0:1] - top)
            fs += [fa, fb]
            mid[g, k, rows:rows + 8, :] = jnp.concatenate([top, fa * a[1:2] + fb * b[1:2], jnp.zeros((6, dim), F32)], axis=0)
        f = jnp.concatenate(fs + [jnp.zeros((dim - 2 * n_x, dim), F32)], axis=0)
        fac[...] = f.T
        for k in range(n_x):
            fcol = fac[lanes(lax.rem(2 * k + c, block), rows), :]
            mid[g, k, 0:rows, :] = msg[g, k, c, 0:rows, :] * fcol[:, 2 * k:2 * k + 1] + got1[g, k, 0:rows, :] * fcol[:, 2 * k + 1:2 * k + 2]
        for i in range(1, n_x):
            copy2(g, i).start()

    def merge2(g):
        for i in range(1, n_x):
            copy2(g, i).wait_recv()
        tiles = [mid[g, x, rows:rows + 8, :]] + [got2[g, i, rows:rows + 8, :] for i in range(1, n_x)]
        m = jnp.concatenate([v[0:1] for v in tiles], axis=0)
        total = jnp.concatenate([v[1:2] for v in tiles], axis=0)
        f = jnp.exp(m - jnp.max(m, axis=0, keepdims=True))
        f = f / jnp.sum(f * total, axis=0, keepdims=True)
        fac[...] = jnp.concatenate([f, jnp.zeros((dim - n_x, dim), F32)], axis=0).T
        fcol = fac[lanes(lax.rem(s, block), rows), :]
        a = mid[g, x, 0:rows, :] * fcol[:, 0:1]
        for i in range(1, n_x):
            a = a + got2[g, i, 0:rows, :] * fcol[:, i:i + 1]
        att[...] = a
        lhs = jnp.concatenate([att[pl.ds(h, own, stride=heads), :] for h in range(heads)], axis=1).astype(BF16)
        part[g] = jnp.dot(lhs, wo[...], preferred_element_type=F32)
        for i in range(1, n_tp):
            copy3(g, i).start()

    def reduce3(g):
        for i in range(1, n_tp):
            copy3(g, i).wait_recv()
        y = part[g, :, lanes(t, cols)]
        for i in range(1, n_tp):
            y = y + got3[g, i]
        y_out[g, x, c, :, lanes(t, cols)] = y
        na, nb = dims(g)
        for i in range(1, na):
            copy4a(g, i).start()
        for i in range(1, nb):
            copy4b(g, 0, i).start()

    def nearest(n):
        return sorted(range(1, n), key=lambda i: min(i, n - i))

    def forward4(g):
        na, nb = dims(g)
        for a in nearest(na):
            copy4a(g, a, a).wait_recv()
            for i in range(1, nb):
                copy4b(g, a, i).start()
        copy4c(g, 0, c).start()

    def collect4(g):
        na, nb = dims(g)
        for i in nearest(nb):
            for a in range(na):
                copy4b(g, a, i, i).wait_recv()
            copy4c(g, i, c).start()

    for g in range(GROUPS):
        copy1(g).start()
    for g in range(GROUPS):
        merge1(g)
    stages = (merge2, reduce3, forward4, collect4)
    for step in range(GROUPS + len(stages) - 1):
        for k, stage in enumerate(stages):
            if 0 <= step - k < GROUPS:
                stage(step - k)
    for g in range(GROUPS):
        na, nb = dims(g)
        for i in range(nb):
            copy4c(g, i, 1 - c).wait_recv()
    for g in range(GROUPS):
        na, nb = dims(g)
        copy1(g).wait_send()
        for i in range(1, n_x):
            copy2(g, i).wait_send()
        for i in range(1, n_tp):
            copy3(g, i).wait_send()
        for i in range(1, na):
            copy4a(g, i).wait_send()
        for a in range(na):
            for i in range(1, nb):
                copy4b(g, a, i).wait_send()
        for i in range(nb):
            copy4c(g, i, c).wait_send()


VM = pl.BlockSpec(memory_space=pltpu.VMEM)
SM = pl.BlockSpec(memory_space=pltpu.SMEM)
ANYW = pl.BlockSpec(memory_space=pl.ANY)
DMA = pltpu.SemaphoreType.DMA


def attend(n_sq, cache_lens, hidden, ln_gain, ln_bias, w_query, b_query, w_kv, b_kv, k_cache, v_cache):
    batch, pos, dim = k_cache.shape
    heads = w_query.shape[1] // dim
    chunks = batch // CHUNK
    rows = batch // GROUPS // n_sq * heads
    return pl.pallas_call(
        functools.partial(attend_kernel, n_sq),
        in_specs=[SM, ANYW, VM, VM, ANYW, VM, ANYW, VM, ANYW, ANYW],
        out_specs=[ANYW, ANYW, VM],
        out_shape=[jax.ShapeDtypeStruct(k_cache.shape, BF16), jax.ShapeDtypeStruct(v_cache.shape, BF16),
                   pltpu.VMEM((GROUPS, n_sq, rows + 8, dim), F32)],
        scratch_shapes=[
            pltpu.VMEM(hidden.shape, BF16), pltpu.VMEM(w_query.shape, BF16), pltpu.VMEM(w_kv.shape, BF16),
            pltpu.VMEM(hidden.shape, BF16), pltpu.VMEM((batch, 2 * dim), F32),
            pltpu.VMEM((batch // 2, 2 * heads, 2 * dim), F32),
            pltpu.VMEM((batch // GROUPS * heads, dim), F32),
            pltpu.VMEM(k_cache.shape, BF16), pltpu.VMEM(v_cache.shape, BF16),
            DMA((3,)), *[DMA((chunks,)) for _ in range(4)],
        ],
        compiler_params=pltpu.CompilerParams(vmem_limit_bytes=54 << 20),
        cost_estimate=pl.CostEstimate(flops=4 * batch * pos * dim * heads * 2, bytes_accessed=4 * k_cache.size, transcendentals=0),
        name="attend",
    )(cache_lens, hidden, ln_gain.reshape(1, -1), ln_bias.reshape(1, -1), w_query, b_query.reshape(1, -1),
      w_kv, b_kv.reshape(1, -1), k_cache, v_cache)


def merge(n_tp, n_sq, batch, heads, msg, w_out):
    dim = msg.shape[-1]
    width = w_out.shape[1]
    own = batch // GROUPS // n_sq
    cols = width // n_tp
    n_x = n_sq // 2
    most = max(n_tp, n_x)
    shapes = [(GROUPS,), (GROUPS, n_x), (GROUPS, n_tp), (GROUPS, most), (GROUPS, most, most), (GROUPS, most)]
    return pl.pallas_call(
        functools.partial(merge_kernel, n_tp, n_sq, heads),
        in_specs=[VM, VM],
        out_specs=VM,
        out_shape=pltpu.VMEM((GROUPS, n_x, 2, own, width), F32),
        scratch_shapes=[
            *[pltpu.VMEM((GROUPS, n_x, *msg.shape[2:]), F32) for _ in range(3)],
            pltpu.VMEM((dim, dim), F32), pltpu.VMEM((own * heads, dim), F32),
            pltpu.VMEM((GROUPS, own, width), F32), pltpu.VMEM((GROUPS, n_tp, own, cols), F32),
            *[DMA(shape) for shape in shapes for _ in range(2)],
        ],
        compiler_params=pltpu.CompilerParams(collective_id=0, has_side_effects=True, vmem_limit_bytes=8 << 20),
        cost_estimate=pl.CostEstimate(flops=40 * batch * 256 * dim * heads, bytes_accessed=4 * batch * width, transcendentals=0),
        name="merge",
    )(msg.reshape(GROUPS, n_x, 2, *msg.shape[2:]), w_out)


def solution(mesh):
    n_tp, n_sq = mesh.shape["tp"], mesh.shape["sq"]

    def local_step(hidden, cache_lens, k_cache, v_cache, ln_gain, ln_bias, w_query, b_query, w_kv, b_kv, w_out, b_out):
        batch, pos, dim = k_cache.shape
        heads = w_query.shape[1] // dim
        key_new, val_new, msg = attend(n_sq, cache_lens, hidden, ln_gain, ln_bias, w_query, b_query, w_kv, b_kv, k_cache, v_cache)
        y = merge(n_tp, n_sq, batch, heads, msg, w_out)
        out_hidden = (hidden.astype(F32) + y.reshape(hidden.shape) + b_out).astype(BF16)
        return out_hidden, key_new, val_new

    cache_spec = P("dp", "sq", None)
    row_spec = P("dp", None)
    in_specs = (row_spec, P("dp"), cache_spec, cache_spec, P(None), P(None), P(None, "tp"), P("tp"), P(None, None), P(None), P("tp", None), P(None))
    return jax.shard_map(local_step, mesh=mesh, in_specs=in_specs, out_specs=(row_spec, cache_spec, cache_spec), check_vma=False)
```

```python
import functools
import jax
import jax.numpy as jnp
from jax import lax
from jax.sharding import PartitionSpec as P
from jax.experimental import pallas as pl
from jax.experimental.pallas import tpu as pltpu

F32 = jnp.float32
BF16 = jnp.bfloat16
MESH = pl.DeviceIdType.MESH
CHUNK = 16
DEPTH = 8
EARLY = 3
GROUPS = 2
LOW = float(jnp.finfo(F32).min)


def attend_kernel(n_sq, lens, hid_h, gain, bias, wq_h, bq, wkv_h, bkv, k_in, v_in,
                  k_out, v_out, msg,
                  hid, wq, wkv, h_scr, kv_scr, qd, stat, k_vm, v_vm, wsem, ksem, vsem, kosem, vosem):
    batch, pos, dim = k_in.shape
    heads = wq.shape[1] // dim
    chunks = batch // CHUNK
    per_group = batch // GROUPS
    own = per_group // n_sq
    rows = own * heads
    first = lax.axis_index("sq") * pos

    wcopies = [pltpu.make_async_copy(src, dst, wsem.at[i])
               for i, (src, dst) in enumerate(((hid_h, hid), (wkv_h, wkv), (wq_h, wq)))]

    def rd(i, src, buf, sem):
        span = pl.ds(i * CHUNK, CHUNK)
        return pltpu.make_async_copy(src.at[span], buf.at[span], sem.at[i])

    def wr(i, buf, dst, sem):
        span = pl.ds(i * CHUNK, CHUNK)
        return pltpu.make_async_copy(buf.at[span], dst.at[span], sem.at[i])

    for copy in wcopies:
        copy.start()

    wcopies[0].wait()
    for i in range(EARLY):
        rd(i, k_in, k_vm, ksem).start()
        rd(i, v_in, v_vm, vsem).start()
    nrow = 32

    def norm_rows(i, _):
        span = pl.ds(pl.multiple_of(i * nrow, nrow), nrow)
        wide = hid[span, :].astype(F32)
        mean = jnp.mean(wide, axis=-1, keepdims=True)
        cent = wide - mean
        var = jnp.mean(cent * cent, axis=-1, keepdims=True)
        normed = cent * lax.rsqrt(var + 1e-5)
        h_scr[span, :] = (normed * gain[...] + bias[...]).astype(BF16)
        return 0

    lax.fori_loop(0, batch // nrow, norm_rows, 0)
    wcopies[1].wait()
    wcopies[2].wait()
    for i in range(EARLY, DEPTH):
        rd(i, k_in, k_vm, ksem).start()
        rd(i, v_in, v_vm, vsem).start()
    kv = jnp.dot(h_scr[...], wkv[...], preferred_element_type=F32) + bkv[...]
    kv_scr[...] = kv.astype(BF16).astype(F32)
    qd[...] = jnp.zeros_like(qd)
    for h in range(heads):
        span = slice(h * dim, (h + 1) * dim)
        q = jnp.dot(h_scr[...], wq[:, span], preferred_element_type=F32) + bq[:, span]
        q = q.astype(BF16).astype(F32).reshape(batch // 2, 2, dim)
        qd[:, h, 0:dim] = q[:, 0, :]
        qd[:, heads + h, dim:2 * dim] = q[:, 1, :]

    pair_rows = 2 * heads
    row = lax.broadcasted_iota(jnp.int32, (pair_rows, pos), 0)
    at = first + lax.broadcasted_iota(jnp.int32, (pair_rows, pos), 1)
    tile_row = lax.broadcasted_iota(jnp.int32, (16, dim), 0)
    lane = lax.broadcasted_iota(jnp.int32, (pair_rows, dim), 1)
    low_half = lax.broadcasted_iota(jnp.int32, (pair_rows, dim), 0) < heads
    pairs = CHUNK // 2
    scale = dim ** -0.5
    per = per_group // CHUNK
    block = dim // rows

    def attend(i, _):
        rd(i, k_in, k_vm, ksem).wait()
        rd(i, v_in, v_vm, vsem).wait()

        @pl.when(i + DEPTH < chunks)
        def _():
            rd(i + DEPTH, k_in, k_vm, ksem).start()
            rd(i + DEPTH, v_in, v_vm, vsem).start()

        base = i * CHUNK
        grp = i // per
        tiles = []
        for j in range(CHUNK):
            slot = lens[base + j] - first
            start = pl.multiple_of((jnp.clip(slot, 0, pos - 1) // 16) * 16, 16)
            hit = tile_row + start == slot
            new = kv_scr[pl.ds(base + j, 1), :]
            kt = k_vm[base + j, pl.ds(start, 16), :].astype(F32)
            vt = v_vm[base + j, pl.ds(start, 16), :].astype(F32)
            tiles.append((start, jnp.where(hit, new[:, :dim], kt).astype(BF16),
                          jnp.where(hit, new[:, dim:], vt).astype(BF16)))
        for j, (start, kt, vt) in enumerate(tiles):
            k_vm[base + j, pl.ds(start, 16), :] = kt
            v_vm[base + j, pl.ds(start, 16), :] = vt
        wr(i, k_vm, k_out, kosem).start()
        wr(i, v_vm, v_out, vosem).start()
        scores = []
        for p in range(pairs):
            b = base + 2 * p
            keys = jnp.concatenate([k_vm[b], k_vm[b + 1]], axis=1)
            q = qd[i * pairs + p].astype(BF16)
            scores.append(lax.dot_general(q, keys, (((1,), (1,)), ((), ())), preferred_element_type=F32) * scale)
        weights = []
        for p in range(pairs):
            b = base + 2 * p
            valid = at <= jnp.where(row < heads, lens[b], lens[b + 1])
            sc = jnp.where(valid, scores[p], LOW)
            m = jnp.max(sc, axis=-1, keepdims=True)
            w = jnp.where(valid, jnp.exp(sc - m), 0.0)
            weights.append((m, jnp.sum(w, axis=-1, keepdims=True), w.astype(BF16)))
        for p in range(pairs):
            b = base + 2 * p
            m, total, w = weights[p]
            vals = jnp.concatenate([v_vm[b], v_vm[b + 1]], axis=1)
            o = jnp.dot(w, vals, preferred_element_type=F32)
            j = lax.rem(b, per_group)
            msg[grp, j // own, pl.ds(pl.multiple_of(lax.rem(j, own) * heads, pair_rows), pair_rows), :] = jnp.where(low_half, o[:, :dim], o[:, dim:])
            stat[pl.ds(pl.multiple_of(j * heads, pair_rows), pair_rows), :] = jnp.where(lane == 0, m, total)
        return 0

    for g in range(GROUPS):
        lax.fori_loop(g * per, (g + 1) * per, attend, 0)
        for a in range(n_sq // block):
            tile = stat[a * dim:(a + 1) * dim, :].T[0:8, :]
            for k in range(block):
                msg[g, a * block + k, rows:rows + 8, :] = tile
    for i in range(chunks):
        wr(i, k_vm, k_out, kosem).wait()
        wr(i, v_vm, v_out, vosem).wait()


def merge_kernel(n_tp, n_sq, heads, msg, wo, y_out, got1, mid, got2, fac, att, part, got3,
                 s1, r1, s2, r2, s3, r3, s4a, r4a, s4b, r4b, s4c, r4c):
    dim = msg.shape[-1]
    own, width = part.shape[1:]
    rows = own * heads
    cols = width // n_tp
    n_x = n_sq // 2
    block = dim // rows
    s = lax.axis_index("sq")
    t = lax.axis_index("tp")
    x, c = s // 2, lax.rem(s, 2)
    partner = {"sq": s + 1 - 2 * c}

    def x_peer(i):
        return {"sq": lax.rem(x + i, n_x) * 2 + c}

    def y_peer(i):
        return {"tp": lax.rem(t + i, n_tp)}

    def remote(src, dst, send, recv, to):
        return pltpu.make_async_remote_copy(src, dst, send, recv, device_id=to, device_id_type=MESH)

    def lanes(k, n):
        return pl.ds(pl.multiple_of(k * n, n), n)

    barrier = pltpu.get_barrier_semaphore()
    pl.semaphore_signal(barrier, inc=1, device_id=partner, device_id_type=MESH)
    for i in range(1, n_x):
        pl.semaphore_signal(barrier, inc=1, device_id=x_peer(i), device_id_type=MESH)
    for i in range(1, n_tp):
        pl.semaphore_signal(barrier, inc=1, device_id=y_peer(i), device_id_type=MESH)
    pl.semaphore_wait(barrier, n_x + n_tp - 1)

    def copy1(g):
        return remote(msg.at[g, :, 1 - c], got1.at[g], s1.at[g], r1.at[g], partner)

    def copy2(g, i):
        return remote(mid.at[g, lax.rem(x + i, n_x)], got2.at[g, i], s2.at[g, i], r2.at[g, i], x_peer(i))

    def copy3(g, i):
        return remote(part.at[g, :, lanes(lax.rem(t + i, n_tp), cols)], got3.at[g, i], s3.at[g, i], r3.at[g, i], y_peer(i))

    def dims(g):
        return (n_x, n_tp) if g % 2 == 0 else (n_tp, n_x)

    def peer(g, second, i):
        return y_peer(i) if (g % 2 == 0) == second else x_peer(i)

    def cell(g, a, b):
        dx, dt = (a, b) if g % 2 == 0 else (b, a)
        return y_out.at[g, lax.rem(x + n_x - dx, n_x), c, :, lanes(lax.rem(t + n_tp - dt, n_tp), cols)]

    def copy4a(g, i, back=0):
        return remote(cell(g, back, 0), cell(g, back, 0), s4a.at[g, i], r4a.at[g, i], peer(g, False, i))

    def copy4b(g, a, i, back=0):
        return remote(cell(g, a, back), cell(g, a, back), s4b.at[g, a, i], r4b.at[g, a, i], peer(g, True, i))

    def copy4c(g, i, core):
        if g % 2 == 0:
            ref = y_out.at[g, :, core, :, lanes(lax.rem(t + n_tp - i, n_tp), cols)]
        else:
            ref = y_out.at[g, lax.rem(x + n_x - i, n_x), core]
        return remote(ref, ref, s4c.at[g, i], r4c.at[g, i], partner)

    def merge1(g):
        copy1(g).wait_recv()
        fs, tiles = [], []
        for k in range(n_x):
            a, b = msg[g, k, c, rows:rows + 8, :], got1[g, k, rows:rows + 8, :]
            top = jnp.maximum(a[0:1], b[0:1])
            fa, fb = jnp.exp(a[0:1] - top), jnp.exp(b[0:1] - top)
            fs += [fa, fb]
            mid[g, k, rows:rows + 8, :] = jnp.concatenate([top, fa * a[1:2] + fb * b[1:2], jnp.zeros((6, dim), F32)], axis=0)
        f = jnp.concatenate(fs + [jnp.zeros((dim - 2 * n_x, dim), F32)], axis=0)
        fac[...] = f.T
        for k in range(n_x):
            fcol = fac[lanes(lax.rem(2 * k + c, block), rows), :]
            mid[g, k, 0:rows, :] = msg[g, k, c, 0:rows, :] * fcol[:, 2 * k:2 * k + 1] + got1[g, k, 0:rows, :] * fcol[:, 2 * k + 1:2 * k + 2]
        for i in range(1, n_x):
            copy2(g, i).start()

    def merge2(g):
        for i in range(1, n_x):
            copy2(g, i).wait_recv()
        tiles = [mid[g, x, rows:rows + 8, :]] + [got2[g, i, rows:rows + 8, :] for i in range(1, n_x)]
        m = jnp.concatenate([v[0:1] for v in tiles], axis=0)
        total = jnp.concatenate([v[1:2] for v in tiles], axis=0)
        f = jnp.exp(m - jnp.max(m, axis=0, keepdims=True))
        f = f / jnp.sum(f * total, axis=0, keepdims=True)
        fac[...] = jnp.concatenate([f, jnp.zeros((dim - n_x, dim), F32)], axis=0).T
        fcol = fac[lanes(lax.rem(s, block), rows), :]
        a = mid[g, x, 0:rows, :] * fcol[:, 0:1]
        for i in range(1, n_x):
            a = a + got2[g, i, 0:rows, :] * fcol[:, i:i + 1]
        att[...] = a
        lhs = jnp.concatenate([att[pl.ds(h, own, stride=heads), :] for h in range(heads)], axis=1).astype(BF16)
        part[g] = jnp.dot(lhs, wo[...], preferred_element_type=F32)
        for i in range(1, n_tp):
            copy3(g, i).start()

    def reduce3(g):
        for i in range(1, n_tp):
            copy3(g, i).wait_recv()
        y = part[g, :, lanes(t, cols)]
        for i in range(1, n_tp):
            y = y + got3[g, i]
        y_out[g, x, c, :, lanes(t, cols)] = y
        na, nb = dims(g)
        for i in range(1, na):
            copy4a(g, i).start()
        for i in range(1, nb):
            copy4b(g, 0, i).start()

    def nearest(n):
        return sorted(range(1, n), key=lambda i: min(i, n - i))

    def forward4(g):
        na, nb = dims(g)
        for a in nearest(na):
            copy4a(g, a, a).wait_recv()
            for i in range(1, nb):
                copy4b(g, a, i).start()
        copy4c(g, 0, c).start()

    def collect4(g):
        na, nb = dims(g)
        for i in nearest(nb):
            for a in range(na):
                copy4b(g, a, i, i).wait_recv()
            copy4c(g, i, c).start()

    for g in range(GROUPS):
        copy1(g).start()
    for g in range(GROUPS):
        merge1(g)
    stages = (merge2, reduce3, forward4, collect4)
    for step in range(GROUPS + len(stages) - 1):
        for k, stage in enumerate(stages):
            if 0 <= step - k < GROUPS:
                stage(step - k)
    for g in range(GROUPS):
        na, nb = dims(g)
        for i in range(nb):
            copy4c(g, i, 1 - c).wait_recv()
    for g in range(GROUPS):
        na, nb = dims(g)
        copy1(g).wait_send()
        for i in range(1, n_x):
            copy2(g, i).wait_send()
        for i in range(1, n_tp):
            copy3(g, i).wait_send()
        for i in range(1, na):
            copy4a(g, i).wait_send()
        for a in range(na):
            for i in range(1, nb):
                copy4b(g, a, i).wait_send()
        for i in range(nb):
            copy4c(g, i, c).wait_send()


VM = pl.BlockSpec(memory_space=pltpu.VMEM)
SM = pl.BlockSpec(memory_space=pltpu.SMEM)
ANYW = pl.BlockSpec(memory_space=pl.ANY)
DMA = pltpu.SemaphoreType.DMA


def attend(n_sq, cache_lens, hidden, ln_gain, ln_bias, w_query, b_query, w_kv, b_kv, k_cache, v_cache):
    batch, pos, dim = k_cache.shape
    heads = w_query.shape[1] // dim
    chunks = batch // CHUNK
    rows = batch // GROUPS // n_sq * heads
    return pl.pallas_call(
        functools.partial(attend_kernel, n_sq),
        in_specs=[SM, ANYW, VM, VM, ANYW, VM, ANYW, VM, ANYW, ANYW],
        out_specs=[ANYW, ANYW, VM],
        out_shape=[jax.ShapeDtypeStruct(k_cache.shape, BF16), jax.ShapeDtypeStruct(v_cache.shape, BF16),
                   pltpu.VMEM((GROUPS, n_sq, rows + 8, dim), F32)],
        scratch_shapes=[
            pltpu.VMEM(hidden.shape, BF16), pltpu.VMEM(w_query.shape, BF16), pltpu.VMEM(w_kv.shape, BF16),
            pltpu.VMEM(hidden.shape, BF16), pltpu.VMEM((batch, 2 * dim), F32),
            pltpu.VMEM((batch // 2, 2 * heads, 2 * dim), F32),
            pltpu.VMEM((batch // GROUPS * heads, dim), F32),
            pltpu.VMEM(k_cache.shape, BF16), pltpu.VMEM(v_cache.shape, BF16),
            DMA((3,)), *[DMA((chunks,)) for _ in range(4)],
        ],
        compiler_params=pltpu.CompilerParams(vmem_limit_bytes=54 << 20),
        cost_estimate=pl.CostEstimate(flops=4 * batch * pos * dim * heads * 2, bytes_accessed=4 * k_cache.size, transcendentals=0),
        name="attend",
    )(cache_lens, hidden, ln_gain.reshape(1, -1), ln_bias.reshape(1, -1), w_query, b_query.reshape(1, -1),
      w_kv, b_kv.reshape(1, -1), k_cache, v_cache)


def merge(n_tp, n_sq, batch, heads, msg, w_out):
    dim = msg.shape[-1]
    width = w_out.shape[1]
    own = batch // GROUPS // n_sq
    cols = width // n_tp
    n_x = n_sq // 2
    most = max(n_tp, n_x)
    shapes = [(GROUPS,), (GROUPS, n_x), (GROUPS, n_tp), (GROUPS, most), (GROUPS, most, most), (GROUPS, most)]
    return pl.pallas_call(
        functools.partial(merge_kernel, n_tp, n_sq, heads),
        in_specs=[VM, VM],
        out_specs=VM,
        out_shape=pltpu.VMEM((GROUPS, n_x, 2, own, width), F32),
        scratch_shapes=[
            *[pltpu.VMEM((GROUPS, n_x, *msg.shape[2:]), F32) for _ in range(3)],
            pltpu.VMEM((dim, dim), F32), pltpu.VMEM((own * heads, dim), F32),
            pltpu.VMEM((GROUPS, own, width), F32), pltpu.VMEM((GROUPS, n_tp, own, cols), F32),
            *[DMA(shape) for shape in shapes for _ in range(2)],
        ],
        compiler_params=pltpu.CompilerParams(collective_id=0, has_side_effects=True, vmem_limit_bytes=8 << 20),
        cost_estimate=pl.CostEstimate(flops=40 * batch * 256 * dim * heads, bytes_accessed=4 * batch * width, transcendentals=0),
        name="merge",
    )(msg.reshape(GROUPS, n_x, 2, *msg.shape[2:]), w_out)


def solution(mesh):
    n_tp, n_sq = mesh.shape["tp"], mesh.shape["sq"]

    def local_step(hidden, cache_lens, k_cache, v_cache, ln_gain, ln_bias, w_query, b_query, w_kv, b_kv, w_out, b_out):
        batch, pos, dim = k_cache.shape
        heads = w_query.shape[1] // dim
        key_new, val_new, msg = attend(n_sq, cache_lens, hidden, ln_gain, ln_bias, w_query, b_query, w_kv, b_kv, k_cache, v_cache)
        y = merge(n_tp, n_sq, batch, heads, msg, w_out)
        out_hidden = (hidden.astype(F32) + y.reshape(hidden.shape) + b_out).astype(BF16)
        return out_hidden, key_new, val_new

    cache_spec = P("dp", "sq", None)
    row_spec = P("dp", None)
    in_specs = (row_spec, P("dp"), cache_spec, cache_spec, P(None), P(None), P(None, "tp"), P("tp"), P(None, None), P(None), P("tp", None), P(None))
    return jax.shard_map(local_step, mesh=mesh, in_specs=in_specs, out_specs=(row_spec, cache_spec, cache_spec), check_vma=False)
```
